256 devices in a mesh: blk: 128 (over x, z, y), rep: 2 (over core).
Axes of the slice: x: 4, y: 4, z: 8, core: 2. Of those that a mesh axis runs over, the one named last changes fastest.
Arguments:
- item_factors: bfloat16 [262144, 256], P('blk')
- user_factors: float32 [2048, 256], P(('blk', 'rep'))
- item_lists: int32 [2048, 128], P(('blk', 'rep')), may hold values from 0 to 262143, as said below
- counts: int32 [2048], P(('blk', 'rep')), may hold values from 16 to 112, as said below
- plays: int32 [2048, 128], P(('blk', 'rep')), may hold values from 0 to 999
Outputs:
- new_factors: float32 [2048, 256], P(('blk', 'rep'))
- residual_norms: float32 [4], replicated
The draws below stay inside these ranges and needn't reach their ends.
Inputs may be any that keep to these rules, and one draw needn't show every extreme that they name: `item_lists`: entries are global item rows; index b of blk holds rows b * 2048 to (b + 1) * 2048 - 1. Among the live slots of the users of one device, at most 8 name rows held by one index of blk, and in every draw some index of blk is named by exactly 8 live slots of every device. The padding slots of one device name rows of every index of blk exactly 4 times. Slots at or after counts[u] are padding. The 8 users of one device have 8 * 64 live slots in all.
All inputs are finite; a program needn't handle non-finite values.
Results may differ from the reference program's by a relative error of at most 0.0003.
Values may be sent and summed in bfloat16 or wider, within the bound.
A program may use at most 64 MiB of HBM per device.

```python
import math
from functools import partial
import jax
import jax.numpy as jnp
import numpy as np
from jax import lax

K = 256
L = 128
U_DEV = 8
I_DEV = 2048
ITERS = 3
USERS = 2048
ITEMS = 262144
N_BLK = 128


def draw_item_factors(key, part):
    key_base, key_cols, key_mix, key_rows = jax.random.split(key, 4)
    base = jax.random.normal(key_base, (ITEMS, K), jnp.float32)
    columns = jnp.exp(jax.random.uniform(key_cols, (K,), jnp.float32, 0.0, math.log(10.0)))
    mixing = jnp.eye(K, dtype=jnp.float32) + 0.5 * jax.random.normal(key_mix, (K, K), jnp.float32) / math.sqrt(K)
    row_scale = jnp.exp(jax.random.uniform(key_rows, (ITEMS, 1), jnp.float32, 0.0, math.log(3.0)))
    mixed = jnp.dot(base * columns[None, :], mixing, precision=lax.Precision.HIGHEST)
    return (mixed * row_scale / (4.0 * math.sqrt(ITEMS))).astype(jnp.bfloat16)


def draw_user_factors(key, part):
    position = jnp.arange(USERS, dtype=jnp.float32) / USERS
    noise = jax.random.normal(key, (USERS, K), jnp.float32)
    scale = 1.0 + 2.0 * position
    return noise * scale[:, None]


def counts_common(key):
    count_key = jax.random.fold_in(key, 7)
    pairs = USERS // 2
    first = jax.random.randint(count_key, (pairs,), L // 8, L - L // 8 + 1)
    first = first.at[0].set(L // 8)
    return jnp.stack([first, L - first], axis=-1).reshape(USERS).astype(jnp.int32)


def draw_counts(key, part):
    return counts_common(key)


def draw_item_lists(key, part):
    device_count = USERS // U_DEV
    slots = U_DEV * L
    live_total = slots // 2
    pad_total = slots - live_total
    average = live_total // N_BLK
    pairs = N_BLK // 2
    key_load, key_pick, key_perm, key_local, key_pad = jax.random.split(jax.random.fold_in(key, 13), 5)
    counts = counts_common(key).reshape(device_count, U_DEV)
    live = (jnp.arange(L, dtype=jnp.int32)[None, None, :] < counts[:, :, None]).reshape(device_count, slots)
    loads_first = jax.random.randint(key_load, (device_count, pairs), 0, 2 * average + 1)
    chosen = jax.random.randint(key_pick, (), 0, pairs)
    loads_first = jnp.where(jnp.arange(pairs)[None, :] == chosen, 2 * average, loads_first)
    loads = jnp.stack([loads_first, 2 * average - loads_first], axis=-1).reshape(device_count, N_BLK)
    ends = jnp.cumsum(loads, axis=1)
    live_positions = jnp.arange(live_total, dtype=jnp.int32)
    live_owners = jax.vmap(lambda edge: jnp.searchsorted(edge, live_positions, side='right'))(ends).astype(jnp.int32)
    perm_keys = jax.random.split(key_perm, device_count)
    live_owners = jax.vmap(lambda pkey, row: row[jax.random.permutation(pkey, live_total)])(perm_keys, live_owners)
    pad_base = jnp.arange(pad_total, dtype=jnp.int32) // (pad_total // N_BLK)
    pad_keys = jax.random.split(key_pad, device_count)
    pad_owners = jax.vmap(lambda pkey: pad_base[jax.random.permutation(pkey, pad_total)])(pad_keys)
    live_index = jnp.cumsum(live.astype(jnp.int32), axis=1) - 1
    pad_index = jnp.cumsum(1 - live.astype(jnp.int32), axis=1) - 1
    live_index = jnp.clip(live_index, 0, live_total - 1)
    pad_index = jnp.clip(pad_index, 0, pad_total - 1)
    owners = jnp.where(live, jnp.take_along_axis(live_owners, live_index, axis=1), jnp.take_along_axis(pad_owners, pad_index, axis=1))
    local = jax.random.randint(key_local, (device_count, slots), 0, I_DEV)
    return (owners * I_DEV + local).astype(jnp.int32).reshape(USERS, L)


def touch_ends(values, own_key, smallest, high):
    longest = values.shape.index(max(values.shape))
    spots = []
    for shift in (0, 1):
        where = [jax.random.randint(jax.random.fold_in(own_key, axis), (), 0, length) for axis, length in enumerate(values.shape)]
        where[longest] = (where[longest] + shift) % values.shape[longest]
        spots.append(tuple(where))
    return values.at[spots[0]].set(smallest).at[spots[1]].set(high)


def rank_bounds(count, skew):
    weights = [(1 << 20) // math.isqrt(rank ** skew) + 1 for rank in range(1, count + 1)]
    scale = 1 + sum(weights) // (1 << 30)
    return np.cumsum(np.array([max(1, weight // scale) for weight in weights]))


def skewed_ids(key, dims, number_of, slope):
    table = rank_bounds(number_of, slope)
    lot = jax.random.randint(jax.random.fold_in(key, 1), dims, 0, int(table[number_of - 1]))
    grade = jnp.searchsorted(jnp.asarray(table, jnp.int32), lot, side="right")
    return jax.random.permutation(jax.random.fold_in(key, 2), number_of)[grade].astype(jnp.int32)


def setup_inputs(seed: int = 0) -> dict:
    arg_keys = jax.random.split(jax.random.key(seed), 6)
    return {
        "item_factors": draw_item_factors(jax.random.fold_in(arg_keys[5], 71), 0),
        "user_factors": draw_user_factors(jax.random.fold_in(arg_keys[5], 71), 0),
        "item_lists": draw_item_lists(jax.random.fold_in(arg_keys[5], 71), 0),
        "counts": draw_counts(jax.random.fold_in(arg_keys[5], 71), 0),
        "plays": touch_ends(skewed_ids(arg_keys[4], (USERS, L), 1000, 2), jax.random.fold_in(arg_keys[4], 3), 0, 999).astype(jnp.int32),
    }


conf_scale = 40.0
ridge = 1.0
tiny = 1e-06

def operator_apply(vector, gram, item_rows, extra_weight):
    along = jnp.einsum('ulk,uk->ul', item_rows, vector, precision=lax.Precision.HIGHEST)
    back = jnp.einsum('ul,ulk->uk', extra_weight * along, item_rows, precision=lax.Precision.HIGHEST)
    return jnp.dot(vector, gram, precision=lax.Precision.HIGHEST) + back + ridge * vector

def solve_block(gram, item_factors, block):
    lists, user_counts, user_plays, start_point = block
    item_rows = item_factors[lists].astype(jnp.float32)
    live = jnp.arange(L, dtype=jnp.int32)[None, :] < user_counts[:, None]
    confidence = 1.0 + conf_scale * jnp.log(2.0 + user_plays.astype(jnp.float32))
    full_weight = jnp.where(live, confidence, jnp.float32(0.0))
    extra_weight = jnp.where(live, confidence - 1.0, jnp.float32(0.0))
    target = jnp.einsum('ul,ulk->uk', full_weight, item_rows, precision=lax.Precision.HIGHEST)
    solution = start_point
    residual = target - operator_apply(solution, gram, item_rows, extra_weight)
    direction = residual
    squares = lax.optimization_barrier(jnp.sum(residual * residual, axis=1))
    collected = [jnp.sum(squares)]
    for _ in range(ITERS):
        image = operator_apply(direction, gram, item_rows, extra_weight)
        alpha = squares / (lax.optimization_barrier(jnp.sum(direction * image, axis=1)) + tiny)
        solution = solution + alpha[:, None] * direction
        residual = residual - alpha[:, None] * image
        fresh = lax.optimization_barrier(jnp.sum(residual * residual, axis=1))
        direction = residual + (fresh / (squares + tiny))[:, None] * direction
        squares = fresh
        collected.append(jnp.sum(squares))
    return (solution, jnp.stack(collected))

def reference(item_factors, user_factors, item_lists, counts, plays):
    gram = lax.dot_general(item_factors, item_factors, (((0,), (0,)), ((), ())), preferred_element_type=jnp.float32)
    block_count = USERS // U_DEV
    shaped = (item_lists.reshape(block_count, U_DEV, L), counts.reshape(block_count, U_DEV), plays.reshape(block_count, U_DEV, L), user_factors.reshape(block_count, U_DEV, K))
    solved, sums = lax.map(partial(solve_block, gram, item_factors), shaped)
    total = lax.optimization_barrier(jnp.sum(sums, axis=0))
    return (solved.reshape(USERS, K), jnp.sqrt(total / (USERS * K)))
```

```python
import jax
import jax.numpy as jnp
from jax import lax
from jax.experimental import pallas as pl
from jax.experimental.pallas import tpu as pltpu
from jax.sharding import Mesh
from jax.sharding import PartitionSpec as P

ITERS = 3
BLK_REP = ("blk_0", "blk_1", "blk_2", "rep")
BLK = ("blk_0", "blk_1", "blk_2")
MESH = pl.DeviceIdType.MESH

NX, NZ, NY, NR = 4, 8, 4, 2
NP = NX * NY
NH = NP * NZ
CAP = 8
U, L, K = 8, 128, 256
ROWS = 2048
USERS = U * NH * NR
F32, BF16, I32 = jnp.float32, jnp.bfloat16, jnp.int32

conf_scale = 40.0
ridge = 1.0
tiny = 1e-06


def dot(a, b):
    return jnp.dot(a, b, preferred_element_type=F32)


def dot_nt(a, b):
    return lax.dot_general(a, b, (((1,), (1,)), ((), ())), preferred_element_type=F32)


def pieces(v):
    hi = v.astype(BF16)
    rest = v - hi.astype(F32)
    mid = rest.astype(BF16)
    low = (rest - mid.astype(F32)).astype(BF16)
    return hi, mid, low


def stacked(v):
    hi, mid, low = pieces(v)
    return jnp.concatenate([hi.astype(F32), mid.astype(F32), low.astype(F32)], axis=0).astype(BF16)


def folded(v, n):
    return v[:n] + v[n : 2 * n] + v[2 * n : 3 * n]


def iota(shape, dim):
    return lax.broadcasted_iota(I32, shape, dim)


def kernel(
    counts_ref,
    lists_ref,
    plays_ref,
    users_ref,
    items_hbm,
    out_ref,
    norms_ref,
    items,
    req_send,
    req_z,
    req_fwd,
    req_p,
    req_t,
    gram_mine,
    gram_p,
    gram_zsend,
    gram_z,
    gram_red,
    gram_full,
    gram3,
    rows_send,
    rows_in,
    rows_mat,
    norm_send,
    norm_p,
    norm_mid,
    norm_z,
    local_sem,
    req_sems,
    gram_sems,
    rows_sem,
    rows_recv,
    norm_sems,
):
    x, z, y, r = (lax.axis_index(a) for a in BLK_REP)
    p = x * NY + y

    def device(pp, zz, rr):
        return (pp // NY, zz, pp % NY, rr)

    def send(src, dst, send_sem, recv_sem, dev):
        pltpu.make_async_remote_copy(
            src_ref=src, dst_ref=dst, send_sem=send_sem, recv_sem=recv_sem, device_id=dev, device_id_type=MESH
        ).start()

    def wait_bytes(ref, sem):
        pltpu.make_async_copy(ref, ref, sem).wait()

    def plane_peer(k):
        both = (p * NR + r + k) % (NP * NR)
        return both // NR, both % NR

    barrier = pltpu.get_barrier_semaphore()

    @pl.loop(1, NP * NR)
    def _(k):
        pp, rr = plane_peer(k)
        pl.semaphore_signal(barrier, inc=1, device_id=device(pp, z, rr), device_id_type=MESH)

    @pl.loop(1, NZ)
    def _(k):
        pl.semaphore_signal(barrier, inc=1, device_id=device(p, (z + k) % NZ, r), device_id_type=MESH)

    items_copy = pltpu.make_async_copy(items_hbm, items, local_sem)
    items_copy.start()

    lists = lists_ref[...]
    user = iota((U, L), 0)
    count = jnp.zeros((U, L), I32)
    for u in range(U):
        count = jnp.where(user == u, counts_ref[u], count)
    live = iota((U, L), 1) < count
    block = lists >> 11
    holder = ((block >> 2) & 7) * NP + (block >> 5) * NY + (block & 3)
    local = lists & (ROWS - 1)
    holder = jnp.where(live, holder, -1)
    before = jnp.where((iota((L, 2 * L), 0) < iota((L, 2 * L), 1)) | (iota((L, 2 * L), 1) >= L), 1.0, 0.0).astype(BF16)
    base = jnp.zeros((NH, L), F32)
    ranks = []
    for u in range(U):
        hit = jnp.where(iota((NH, L), 0) == holder[u : u + 1, :], 1.0, 0.0)
        sums = dot(hit.astype(BF16), before)
        ranks.append(jnp.sum(hit * (sums[:, :L] + base), axis=0, keepdims=True))
        base = base + sums[:, L:]
    rank = jnp.concatenate(ranks, axis=0)
    place = jnp.where(live, holder.astype(F32) * CAP + rank, -1.0)
    place_t = jnp.concatenate([place, jnp.zeros((L - U, L), F32)], axis=0).T

    confidence = 1.0 + conf_scale * jnp.log(2.0 + plays_ref[...].astype(F32))
    full_weight = jnp.where(live, confidence, 0.0)
    full3 = [v.astype(F32) for v in pieces(full_weight)]
    id_hi = (local >> 4).astype(F32)
    id_lo = (local & 15).astype(F32)
    found = jnp.zeros((4 * U, NH * CAP), F32)
    for u in range(U):
        pick = jnp.where(place_t[:, u : u + 1] == iota((L, NH * CAP), 1).astype(F32), 1.0, 0.0).astype(BF16)
        names = jnp.where(user == 0, id_hi[u : u + 1, :], jnp.where(user == 1, id_lo[u : u + 1, :], 0.0))
        left = jnp.concatenate([jnp.where(user == u, v, 0.0) for v in full3] + [names], axis=0).astype(BF16)
        found = found + dot(left, pick)
    weight = folded(found, U)
    extra = jnp.where(weight > 0.0, weight - 1.0, 0.0)
    wanted = found[3 * U : 3 * U + 1] * 16.0 + found[3 * U + 1 : 3 * U + 2]
    for k in range(NZ):
        req_send[k] = wanted[:, k * L : (k + 1) * L]
    req_z[z] = req_send[z]

    pl.semaphore_wait(barrier, NP * NR - 1 + NZ - 1)

    @pl.loop(1, NZ)
    def _(k):
        zz = (z + k) % NZ
        send(req_send.at[zz], req_z.at[z], req_sems.at[0], req_sems.at[1], device(p, zz, r))

    items_copy.wait()
    half = pl.ds(pl.multiple_of(r * (K // NR), K // NR), K // NR)
    part = lax.dot_general(items[:, half], items[...], (((0,), (0,)), ((), ())), preferred_element_type=F32)
    gram_mine[...] = part.reshape(NP, 8, K)
    gram_p[p] = gram_mine[p]

    @pl.loop(1, NP)
    def _(k):
        pp = (p + k) % NP
        send(gram_mine.at[pp], gram_p.at[p], gram_sems.at[0], gram_sems.at[1], device(pp, z, r))

    wait_bytes(req_send.at[pl.ds(0, NZ - 1)], req_sems.at[0])
    wait_bytes(req_z.at[pl.ds(0, NZ - 1)], req_sems.at[1])
    req_fwd[...] = req_z[...].reshape(NZ, L)
    req_p[p] = req_fwd[...]

    @pl.loop(1, NP)
    def _(k):
        send(req_fwd, req_p.at[p], req_sems.at[2], req_sems.at[3], device((p + k) % NP, z, r))

    wait_bytes(gram_mine.at[pl.ds(0, NP - 1)], gram_sems.at[0])
    wait_bytes(gram_p.at[pl.ds(0, NP - 1)], gram_sems.at[1])
    gram_zsend[...] = jnp.sum(gram_p[...], axis=0)
    gram_z[z] = gram_zsend[...]

    @pl.loop(1, NZ)
    def _(k):
        send(gram_zsend, gram_z.at[z], gram_sems.at[2], gram_sems.at[3], device(p, (z + k) % NZ, r))

    wait_bytes(req_p.at[pl.ds(0, NP - 1)], req_sems.at[2])
    wait_bytes(req_p.at[pl.ds(0, NP - 1)], req_sems.at[3])
    req_t[...] = req_p[...].reshape(NP * NZ, L).T
    asked = req_t[pl.ds(pl.multiple_of(p * CAP, CAP), CAP), :]
    first = 3
    asked = pltpu.roll(asked, (L - z - first) % L, axis=1)

    def serve(step, asked):
        column = jnp.concatenate([asked[:, i * NZ : i * NZ + 1] for i in range(NP)], axis=0)
        total = jnp.zeros((NP * CAP, K), F32)
        width = 512
        for part in range(ROWS // width):
            pick = jnp.where(column == (iota((NP * CAP, width), 1) + part * width).astype(F32), 1.0, 0.0).astype(BF16)
            total = total + dot(pick, items[part * width : (part + 1) * width, :])
        rows_send[pl.ds(pl.multiple_of(step * NP, NP), NP)] = total.reshape(NP, CAP, K).astype(BF16)

        @pl.loop(0, NP)
        def _(i):
            to = (i * NZ + step + z + first) % (NP * NZ)
            pp, zz = to // NZ, to % NZ
            mine = to == p * NZ + z
            src = rows_send.at[step * NP + i]
            dst = rows_in.at[z * NP + p]

            @pl.when(mine)
            def _():
                pltpu.make_async_copy(src, dst, rows_recv.at[z]).start()

            @pl.when(jnp.logical_not(mine))
            def _():
                send(src, dst, rows_sem, rows_recv.at[z], device(pp, zz, r))

        return pltpu.roll(asked, L - 1, axis=1)

    lax.fori_loop(0, NZ, serve, asked)

    wait_bytes(gram_z.at[pl.ds(0, NZ - 1)], gram_sems.at[2])
    wait_bytes(gram_z.at[pl.ds(0, NZ - 1)], gram_sems.at[3])
    gram_red[...] = jnp.sum(gram_z[...], axis=0)
    gram_full[r * NP + p] = gram_red[...]

    @pl.loop(1, NP * NR)
    def _(k):
        pp, rr = plane_peer(k)
        send(gram_red, gram_full.at[r * NP + p], gram_sems.at[4], gram_sems.at[5], device(pp, z, rr))

    wait_bytes(gram_full.at[pl.ds(0, NP * NR - 1)], gram_sems.at[4])
    wait_bytes(gram_full.at[pl.ds(0, NP * NR - 1)], gram_sems.at[5])
    for k, piece in enumerate(pieces(gram_full[...].reshape(K, K))):
        gram3[:, k * K : (k + 1) * K] = piece

    for k in range(NZ):
        wait_bytes(rows_in.at[pl.ds(k * NP, NP)], rows_recv.at[k])
        rows_mat[k * L : (k + 1) * L, :] = rows_in[k * NP : (k + 1) * NP].astype(F32).reshape(L, K).astype(BF16)
    wait_bytes(rows_send.at[pl.ds(0, NH - 1)], rows_sem)

    def image_of(v):
        v3 = stacked(v)
        along = folded(dot_nt(v3, rows_mat[...]), U)
        back = folded(dot(stacked(extra * along), rows_mat[...]), U)
        g = folded(dot(v3, gram3[...]), U)
        return g[:, :K] + g[:, K : 2 * K] + g[:, 2 * K :] + back + ridge * v

    def inner(a, b):
        return jnp.sum(a * b, axis=1, keepdims=True)

    target = folded(dot(stacked(weight), rows_mat[...]), U)
    solution = users_ref[...]
    residual = target - image_of(solution)
    direction = residual
    squares = inner(residual, residual)
    lane = iota((U, L), 1)
    collected = jnp.where(lane == 0, squares, 0.0)
    for t in range(ITERS):
        image = image_of(direction)
        alpha = squares / (inner(direction, image) + tiny)
        solution = solution + alpha * direction
        residual = residual - alpha * image
        fresh = inner(residual, residual)
        direction = residual + (fresh / (squares + tiny)) * direction
        squares = fresh
        collected = collected + jnp.where(lane == t + 1, squares, 0.0)
    out_ref[...] = solution

    norm_send[...] = jnp.sum(collected, axis=0, keepdims=True)
    norm_p[p * NR + r] = norm_send[...]

    @pl.loop(1, NP * NR)
    def _(k):
        pp, rr = plane_peer(k)
        send(norm_send, norm_p.at[p * NR + r], norm_sems.at[0], norm_sems.at[1], device(pp, z, rr))

    wait_bytes(norm_p.at[pl.ds(0, NP * NR - 1)], norm_sems.at[0])
    wait_bytes(norm_p.at[pl.ds(0, NP * NR - 1)], norm_sems.at[1])
    norm_mid[...] = jnp.sum(norm_p[...], axis=0)
    norm_z[z] = norm_mid[...]

    @pl.loop(1, NZ)
    def _(k):
        send(norm_mid, norm_z.at[z], norm_sems.at[2], norm_sems.at[3], device(p, (z + k) % NZ, r))

    wait_bytes(norm_z.at[pl.ds(0, NZ - 1)], norm_sems.at[2])
    wait_bytes(norm_z.at[pl.ds(0, NZ - 1)], norm_sems.at[3])
    total = jnp.sum(norm_z[...], axis=0)
    norms_ref[...] = jnp.sqrt(total / (USERS * K))[:, : ITERS + 1]


def body(item_factors, user_factors, item_lists, counts, plays):
    vmem = pl.BlockSpec(memory_space=pltpu.VMEM)
    dma = pltpu.SemaphoreType.DMA
    new_factors, norms = pl.pallas_call(
        kernel,
        out_shape=(jax.ShapeDtypeStruct((U, K), F32), jax.ShapeDtypeStruct((1, ITERS + 1), F32)),
        in_specs=[pl.BlockSpec(memory_space=pltpu.SMEM), vmem, vmem, vmem, pl.BlockSpec(memory_space=pl.ANY)],
        out_specs=(vmem, vmem),
        scratch_shapes=[
            pltpu.VMEM((ROWS, K), BF16),
            pltpu.VMEM((NZ, 1, L), F32),
            pltpu.VMEM((NZ, 1, L), F32),
            pltpu.VMEM((NZ, L), F32),
            pltpu.VMEM((NP, NZ, L), F32),
            pltpu.VMEM((L, NP * NZ), F32),
            pltpu.VMEM((NP, 8, K), F32),
            pltpu.VMEM((NP, 8, K), F32),
            pltpu.VMEM((8, K), F32),
            pltpu.VMEM((NZ, 8, K), F32),
            pltpu.VMEM((8, K), F32),
            pltpu.VMEM((NR * NP, 8, K), F32),
            pltpu.VMEM((K, 3 * K), BF16),
            pltpu.VMEM((NH, CAP, K), BF16),
            pltpu.VMEM((NH, CAP, K), BF16),
            pltpu.VMEM((NH * CAP, K), BF16),
            pltpu.VMEM((1, L), F32),
            pltpu.VMEM((NP * NR, 1, L), F32),
            pltpu.VMEM((1, L), F32),
            pltpu.VMEM((NZ, 1, L), F32),
            dma,
            dma((4,)),
            dma((6,)),
            dma,
            dma((NZ,)),
            dma((4,)),
        ],
        compiler_params=pltpu.CompilerParams(collective_id=0, has_side_effects=True),
    )(counts, item_lists, plays, user_factors, item_factors)
    return new_factors, norms.reshape(ITERS + 1)


def solution(mesh):
    split = Mesh(mesh.devices.reshape(NX, NZ, NY, NR), BLK_REP)
    in_specs = (P(BLK, None), P(BLK_REP, None), P(BLK_REP, None), P(BLK_REP), P(BLK_REP, None))
    out_specs = (P(BLK_REP, None), P())
    return jax.shard_map(body, mesh=split, in_specs=in_specs, out_specs=out_specs, check_vma=False)
```

```python
import jax
import jax.numpy as jnp
from jax import lax
from jax.experimental import pallas as pl
from jax.experimental.pallas import tpu as pltpu
from jax.sharding import Mesh
from jax.sharding import PartitionSpec as P

ITERS = 3
BLK_REP = ("blk_0", "blk_1", "blk_2", "rep")
BLK = ("blk_0", "blk_1", "blk_2")
MESH = pl.DeviceIdType.MESH

NX, NZ, NY, NR = 4, 8, 4, 2
NP = NX * NY
NH = NP * NZ
CAP = 8
U, L, K = 8, 128, 256
ROWS = 2048
USERS = U * NH * NR
GRAM_AFTER = 2
F32, BF16, I32 = jnp.float32, jnp.bfloat16, jnp.int32

conf_scale = 40.0
ridge = 1.0
tiny = 1e-06


def dot(a, b):
    return jnp.dot(a, b, preferred_element_type=F32)


def dot_nt(a, b):
    return lax.dot_general(a, b, (((1,), (1,)), ((), ())), preferred_element_type=F32)


def pieces(v):
    hi = v.astype(BF16)
    rest = v - hi.astype(F32)
    mid = rest.astype(BF16)
    low = (rest - mid.astype(F32)).astype(BF16)
    return hi, mid, low


def stacked(v):
    hi, mid, low = pieces(v)
    return jnp.concatenate([hi.astype(F32), mid.astype(F32), low.astype(F32)], axis=0).astype(BF16)


def folded(v, n):
    return v[:n] + v[n : 2 * n] + v[2 * n : 3 * n]


def iota(shape, dim):
    return lax.broadcasted_iota(I32, shape, dim)


class Phases:
    def __init__(self):
        self.open = None

    def __call__(self, name):
        if self.open is not None:
            self.open.__exit__(None, None, None)
        self.open = jax.named_scope(name) if name else None
        if self.open is not None:
            self.open.__enter__()


NEAR = sorted(((dx, dy) for dx in range(NX) for dy in range(NY)), key=lambda d: (min(d[0], NX - d[0]) + min(d[1], NY - d[1]), d))
FAR_Z = (4, 3, 5, 2, 6, 1, 7, 0)


def kernel(
    counts_hbm,
    lists_hbm,
    plays_hbm,
    users_hbm,
    items_hbm,
    out_ref,
    norms_ref,
    counts_ref,
    lists_ref,
    plays_ref,
    users_ref,
    items,
    req_send,
    req_z,
    req_fwd,
    req_p,
    gram_mine,
    gram_p,
    gram_zsend,
    gram_z,
    gram_red,
    gram_full,
    gram3,
    rows_send,
    rows_in,
    rows_mat,
    norm_send,
    norm_p,
    norm_mid,
    norm_z,
    local_sems,
    req_sems,
    req_recv,
    gram_sems,
    rows_sem,
    rows_recv,
    norm_sems,
):
    phase = Phases()
    phase("enter")
    x, z, y, r = (lax.axis_index(a) for a in BLK_REP)
    p = x * NY + y

    def plane_device(d, same=1):
        return ((x + d[0]) & (NX - 1), z, (y + d[1]) & (NY - 1), r if same else 1 - r)

    def z_device(dz):
        return (x, (z + dz) & (NZ - 1), y, r)

    def place_of(dev):
        return dev[0] * NY + dev[2]

    peers = [(d, same) for same in (1, 0) for d in reversed(NEAR) if not (same and d == (0, 0))]

    def send(src, dst, send_sem, recv_sem, dev):
        pltpu.make_async_remote_copy(
            src_ref=src, dst_ref=dst, send_sem=send_sem, recv_sem=recv_sem, device_id=dev, device_id_type=MESH
        ).start()

    def wait_bytes(ref, sem):
        pltpu.make_async_copy(ref, ref, sem).wait()

    copies = [
        pltpu.make_async_copy(src, dst, local_sems.at[k])
        for k, (src, dst) in enumerate(
            [(counts_hbm, counts_ref), (lists_hbm, lists_ref), (plays_hbm, plays_ref), (users_hbm, users_ref), (items_hbm, items)]
        )
    ]
    for copy in copies:
        copy.start()
    barrier = pltpu.get_barrier_semaphore()
    for dz in range(1, NZ):
        pl.semaphore_signal(barrier, inc=1, device_id=z_device(dz), device_id_type=MESH)
    for d, same in peers:
        pl.semaphore_signal(barrier, inc=1, device_id=plane_device(d, same), device_id_type=MESH)
    for copy in copies[:3]:
        copy.wait()

    phase("pack")
    lists = lists_ref[...]
    user = iota((U, L), 0)
    count = jnp.zeros((U, L), I32)
    for u in range(U):
        count = jnp.where(user == u, counts_ref[u], count)
    live = iota((U, L), 1) < count
    block = lists >> 11
    holder = ((block >> 2) & 7) * NP + (block >> 5) * NY + (block & 3)
    local = lists & (ROWS - 1)
    holder = jnp.where(live, holder, -1)
    before = jnp.where((iota((L, 2 * L), 0) < iota((L, 2 * L), 1)) | (iota((L, 2 * L), 1) >= L), 1.0, 0.0).astype(BF16)
    base = jnp.zeros((NH, L), F32)
    ranks = []
    for u in range(U):
        hit = jnp.where(iota((NH, L), 0) == holder[u : u + 1, :], 1.0, 0.0)
        sums = dot(hit.astype(BF16), before)
        ranks.append(jnp.sum(hit * (sums[:, :L] + base), axis=0, keepdims=True))
        base = base + sums[:, L:]
    rank = jnp.concatenate(ranks, axis=0)
    place = jnp.where(live, holder.astype(F32) * CAP + rank, -1.0)
    place_t = jnp.concatenate([place, jnp.zeros((L - U, L), F32)], axis=0).T

    phase("weights")
    confidence = 1.0 + conf_scale * jnp.log(2.0 + plays_ref[...].astype(F32))
    full_weight = jnp.where(live, confidence, 0.0)
    full3 = [v.astype(F32) for v in pieces(full_weight)]
    id_hi = (local >> 4).astype(F32)
    id_lo = (local & 15).astype(F32)
    found = jnp.zeros((4 * U, NH * CAP), F32)
    for u in range(U):
        pick = jnp.where(place_t[:, u : u + 1] == iota((L, NH * CAP), 1).astype(F32), 1.0, 0.0).astype(BF16)
        names = jnp.where(user == 0, id_hi[u : u + 1, :], jnp.where(user == 1, id_lo[u : u + 1, :], 0.0))
        left = jnp.concatenate([jnp.where(user == u, v, 0.0) for v in full3] + [names], axis=0).astype(BF16)
        found = found + dot(left, pick)
    weight = folded(found, U)
    extra = jnp.where(weight > 0.0, weight - 1.0, 0.0)
    wanted = found[3 * U : 3 * U + 1] * 16.0 + found[3 * U + 1 : 3 * U + 2]
    for k in range(NZ):
        req_send[k] = wanted[:, k * L : (k + 1) * L]
    req_z[0] = req_send[z]

    phase("barrier")
    pl.semaphore_wait(barrier, NP * NR - 1 + NZ - 1)
    for dz in FAR_Z[:-1]:
        dev = z_device(dz)
        send(req_send.at[dev[1]], req_z.at[NZ - dz], req_sems.at[0], req_sems.at[1], dev)

    phase("gram")
    copies[4].wait()
    half = pl.ds(pl.multiple_of(r * (K // NR), K // NR), K // NR)
    part = lax.dot_general(items[:, half], items[...], (((0,), (0,)), ((), ())), preferred_element_type=F32)
    gram_mine[...] = part.reshape(NP, 8, K)
    gram_p[p] = gram_mine[p]
    phase("gram_p_send")
    for d in reversed(NEAR[1:]):
        dev = plane_device(d)
        send(gram_mine.at[place_of(dev)], gram_p.at[p], gram_sems.at[0], gram_sems.at[1], dev)

    phase("req_z_wait")
    wait_bytes(req_z.at[pl.ds(0, NZ - 1)], req_sems.at[1])
    req_fwd[...] = jnp.concatenate([req_z[...].reshape(NZ, L), jnp.zeros((L - NZ, L), F32)], axis=0).T.reshape(NP, CAP, L)
    phase("req_p_send")
    for k in reversed(range(1, NP)):
        dev = plane_device(NEAR[k])
        send(req_fwd.at[place_of(dev)], req_p.at[k], req_sems.at[2], req_recv.at[k], dev)

    phase("gram_p_wait")
    wait_bytes(gram_p.at[pl.ds(0, NP - 1)], gram_sems.at[1])
    gram_zsend[...] = jnp.sum(gram_p[...], axis=0)
    gram_z[z] = gram_zsend[...]
    for dz in FAR_Z[:-1]:
        send(gram_zsend, gram_z.at[z], gram_sems.at[2], gram_sems.at[3], z_device(dz))

    def serve(step):
        tiles = []
        for k in (2 * step, 2 * step + 1):
            if k:
                wait_bytes(req_p.at[k], req_recv.at[k])
            tiles.append(req_p[k] if k else req_fwd[p])
        column = jnp.concatenate([t[:, dz : dz + 1] for t in tiles for dz in FAR_Z], axis=0)
        total = jnp.zeros((2 * NZ * CAP, K), F32)
        width = 512
        for part in range(ROWS // width):
            pick = jnp.where(column == (iota((2 * NZ * CAP, width), 1) + part * width).astype(F32), 1.0, 0.0).astype(BF16)
            total = total + dot(pick, items[part * width : (part + 1) * width, :])
        rows_send[step] = total.reshape(2 * NZ, CAP, K).astype(BF16)
        for i in range(2):
            d = NEAR[2 * step + i]
            for j, dz in enumerate(FAR_Z):
                dev = ((x - d[0]) & (NX - 1), (z + dz) & (NZ - 1), (y - d[1]) & (NY - 1), r)
                src = rows_send.at[step, i * NZ + j]
                dst = rows_in.at[z * NP + p]
                if d == (0, 0) and dz == 0:
                    pltpu.make_async_copy(src, dst, rows_recv).start()
                else:
                    send(src, dst, rows_sem, rows_recv, dev)

    def spread_gram():
        wait_bytes(gram_z.at[pl.ds(0, NZ - 1)], gram_sems.at[3])
        gram_red[...] = jnp.sum(gram_z[...], axis=0)
        gram_full[r * NP + p] = gram_red[...]
        for d, same in peers:
            send(gram_red, gram_full.at[r * NP + p], gram_sems.at[4], gram_sems.at[5], plane_device(d, same))

    for step in range(NP // 2):
        phase("serve%d" % step)
        serve(step)
        if step == GRAM_AFTER:
            phase("gram_ag")
            spread_gram()

    phase("gram_ag_wait")
    wait_bytes(gram_full.at[pl.ds(0, NP * NR - 1)], gram_sems.at[5])
    phase("gram_pieces")
    for k, piece in enumerate(pieces(gram_full[...].reshape(K, K))):
        gram3[:, k * K : (k + 1) * K] = piece

    phase("rows_wait")
    wait_bytes(rows_in, rows_recv)
    rows_mat[...] = rows_in[...].astype(F32).reshape(NH * CAP, K).astype(BF16)

    phase("cg")
    def image_of(v):
        v3 = stacked(v)
        along = folded(dot_nt(v3, rows_mat[...]), U)
        back = folded(dot(stacked(extra * along), rows_mat[...]), U)
        g = folded(dot(v3, gram3[...]), U)
        return g[:, :K] + g[:, K : 2 * K] + g[:, 2 * K :] + back + ridge * v

    def inner(a, b):
        return jnp.sum(a * b, axis=1, keepdims=True)

    target = folded(dot(stacked(weight), rows_mat[...]), U)
    copies[3].wait()
    solution = users_ref[...]
    residual = target - image_of(solution)
    direction = residual
    squares = inner(residual, residual)
    lane = iota((U, L), 1)
    collected = jnp.where(lane == 0, squares, 0.0)
    for t in range(ITERS):
        image = image_of(direction)
        alpha = squares / (inner(direction, image) + tiny)
        solution = solution + alpha * direction
        residual = residual - alpha * image
        fresh = inner(residual, residual)
        direction = residual + (fresh / (squares + tiny)) * direction
        squares = fresh
        collected = collected + jnp.where(lane == t + 1, squares, 0.0)

    norm_send[...] = jnp.sum(collected, axis=0, keepdims=True)
    phase("norm_p")
    norm_p[p * NR + r] = norm_send[...]
    for d, same in peers:
        send(norm_send, norm_p.at[p * NR + r], norm_sems.at[0], norm_sems.at[1], plane_device(d, same))
    out_ref[...] = solution
    wait_bytes(req_z.at[pl.ds(0, NZ - 1)], req_sems.at[0])
    wait_bytes(req_p.at[pl.ds(0, NP - 1)], req_sems.at[2])
    wait_bytes(gram_mine.at[pl.ds(0, NP - 1)], gram_sems.at[0])
    wait_bytes(gram_z.at[pl.ds(0, NZ - 1)], gram_sems.at[2])
    wait_bytes(gram_full.at[pl.ds(0, NP * NR - 1)], gram_sems.at[4])
    wait_bytes(rows_in.at[pl.ds(0, NH - 1)], rows_sem)
    wait_bytes(norm_p.at[pl.ds(0, NP * NR - 1)], norm_sems.at[1])
    norm_mid[...] = jnp.sum(norm_p[...], axis=0)
    phase("norm_z")
    norm_z[z] = norm_mid[...]
    for dz in FAR_Z[:-1]:
        send(norm_mid, norm_z.at[z], norm_sems.at[2], norm_sems.at[3], z_device(dz))
    wait_bytes(norm_p.at[pl.ds(0, NP * NR - 1)], norm_sems.at[0])
    wait_bytes(norm_z.at[pl.ds(0, NZ - 1)], norm_sems.at[3])
    phase("norm_end")
    total = jnp.sum(norm_z[...], axis=0)
    norms_ref[...] = jnp.sqrt(total / (USERS * K))[:, : ITERS + 1]
    wait_bytes(norm_z.at[pl.ds(0, NZ - 1)], norm_sems.at[2])
    phase(None)


def body(item_factors, user_factors, item_lists, counts, plays):
    vmem = pl.BlockSpec(memory_space=pltpu.VMEM)
    dma = pltpu.SemaphoreType.DMA
    new_factors, norms = pl.pallas_call(
        kernel,
        out_shape=(jax.ShapeDtypeStruct((U, K), F32), jax.ShapeDtypeStruct((1, ITERS + 1), F32)),
        in_specs=[pl.BlockSpec(memory_space=pl.ANY)] * 5,
        out_specs=(vmem, vmem),
        scratch_shapes=[
            pltpu.SMEM((U,), I32),
            pltpu.VMEM((U, L), I32),
            pltpu.VMEM((U, L), I32),
            pltpu.VMEM((U, K), F32),
            pltpu.VMEM((ROWS, K), BF16),
            pltpu.VMEM((NZ, 1, L), F32),
            pltpu.VMEM((NZ, 1, L), F32),
            pltpu.VMEM((NP, CAP, L), F32),
            pltpu.VMEM((NP, CAP, L), F32),
            pltpu.VMEM((NP, 8, K), F32),
            pltpu.VMEM((NP, 8, K), F32),
            pltpu.VMEM((8, K), F32),
            pltpu.VMEM((NZ, 8, K), F32),
            pltpu.VMEM((8, K), F32),
            pltpu.VMEM((NR * NP, 8, K), F32),
            pltpu.VMEM((K, 3 * K), BF16),
            pltpu.VMEM((NP // 2, 2 * NZ, CAP, K), BF16),
            pltpu.VMEM((NH, CAP, K), BF16),
            pltpu.VMEM((NH * CAP, K), BF16),
            pltpu.VMEM((1, L), F32),
            pltpu.VMEM((NP * NR, 1, L), F32),
            pltpu.VMEM((1, L), F32),
            pltpu.VMEM((NZ, 1, L), F32),
            dma((5,)),
            dma((3,)),
            dma((NP,)),
            dma((6,)),
            dma,
            dma,
            dma((4,)),
        ],
        compiler_params=pltpu.CompilerParams(collective_id=0, has_side_effects=True),
    )(counts, item_lists, plays, user_factors, item_factors)
    return new_factors, norms.reshape(ITERS + 1)


def solution(mesh):
    split = Mesh(mesh.devices.reshape(NX, NZ, NY, NR), BLK_REP)
    in_specs = (P(BLK, None), P(BLK_REP, None), P(BLK_REP, None), P(BLK_REP), P(BLK_REP, None))
    out_specs = (P(BLK_REP, None), P())
    return jax.shard_map(body, mesh=split, in_specs=in_specs, out_specs=out_specs, check_vma=False)
```

```python
import jax
import jax.numpy as jnp
from jax import lax
from jax.experimental import pallas as pl
from jax.experimental.pallas import tpu as pltpu
from jax.sharding import Mesh
from jax.sharding import PartitionSpec as P

ITERS = 3
BLK_REP = ("blk_0", "blk_1", "blk_2", "rep")
BLK = ("blk_0", "blk_1", "blk_2")
MESH = pl.DeviceIdType.MESH

NX, NZ, NY, NR = 4, 8, 4, 2
NP = NX * NY
NH = NP * NZ
CAP = 8
U, L, K = 8, 128, 256
ROWS = 2048
USERS = U * NH * NR
GRAM_AFTER = 2
F32, BF16, I32 = jnp.float32, jnp.bfloat16, jnp.int32

conf_scale = 40.0
ridge = 1.0
tiny = 1e-06


def dot(a, b):
    return jnp.dot(a, b, preferred_element_type=F32)


def dot_nt(a, b):
    return lax.dot_general(a, b, (((1,), (1,)), ((), ())), preferred_element_type=F32)


def pieces(v):
    hi = v.astype(BF16)
    rest = v - hi.astype(F32)
    mid = rest.astype(BF16)
    low = (rest - mid.astype(F32)).astype(BF16)
    return hi, mid, low


def stacked(v):
    hi, mid, low = pieces(v)
    return jnp.concatenate([hi.astype(F32), mid.astype(F32), low.astype(F32)], axis=0).astype(BF16)


def folded(v, n):
    return v[:n] + v[n : 2 * n] + v[2 * n : 3 * n]


def iota(shape, dim):
    return lax.broadcasted_iota(I32, shape, dim)


class Phases:
    def __init__(self):
        self.open = None

    def __call__(self, name):
        if self.open is not None:
            self.open.__exit__(None, None, None)
        self.open = jax.named_scope(name) if name else None
        if self.open is not None:
            self.open.__enter__()


NEAR = sorted(((dx, dy) for dx in range(NX) for dy in range(NY)), key=lambda d: (min(d[0], NX - d[0]) + min(d[1], NY - d[1]), d))
EVERY = sorted(
    ((d, dz) for d in NEAR for dz in range(NZ) if d != (0, 0) or dz),
    key=lambda o: -(min(o[0][0], NX - o[0][0]) + min(o[0][1], NY - o[0][1]) + min(o[1], NZ - o[1])),
)
STEPS = (0, 7, 6, 5, 4, 3, 2, 1)
FAR_Z = (4, 3, 5, 2, 6, 1, 7, 0)


def kernel(
    counts_hbm,
    lists_hbm,
    plays_hbm,
    users_hbm,
    items_hbm,
    out_ref,
    norms_ref,
    counts_ref,
    lists_ref,
    plays_ref,
    users_ref,
    items,
    req_send,
    req_z,
    req_fwd,
    req_p,
    gram_mine,
    gram_p,
    gram_zsend,
    gram_z,
    gram_red,
    gram_full,
    gram3,
    rows_send,
    rows_in,
    rows_mat,
    norm_send,
    norm_pair,
    norm_mid,
    norm_all,
    local_sems,
    req_sems,
    req_recv,
    gram_sems,
    rows_sem,
    rows_recv,
    norm_sems,
):
    phase = Phases()
    phase("enter")
    x, z, y, r = (lax.axis_index(a) for a in BLK_REP)
    p = x * NY + y

    def plane_device(d, same=1):
        return ((x + d[0]) & (NX - 1), z, (y + d[1]) & (NY - 1), r if same else 1 - r)

    def z_device(dz):
        return (x, (z + dz) & (NZ - 1), y, r)

    def place_of(dev):
        return dev[0] * NY + dev[2]

    peers = [(d, same) for same in (1, 0) for d in reversed(NEAR) if not (same and d == (0, 0))]

    def send(src, dst, send_sem, recv_sem, dev):
        pltpu.make_async_remote_copy(
            src_ref=src, dst_ref=dst, send_sem=send_sem, recv_sem=recv_sem, device_id=dev, device_id_type=MESH
        ).start()

    def wait_bytes(ref, sem):
        pltpu.make_async_copy(ref, ref, sem).wait()

    copies = [
        pltpu.make_async_copy(src, dst, local_sems.at[k])
        for k, (src, dst) in enumerate(
            [(counts_hbm, counts_ref), (lists_hbm, lists_ref), (plays_hbm, plays_ref), (users_hbm, users_ref), (items_hbm, items)]
        )
    ]
    for copy in copies:
        copy.start()
    barrier = pltpu.get_barrier_semaphore()
    for dz in range(1, NZ):
        pl.semaphore_signal(barrier, inc=1, device_id=z_device(dz), device_id_type=MESH)
    for d, same in peers:
        pl.semaphore_signal(barrier, inc=1, device_id=plane_device(d, same), device_id_type=MESH)
    for copy in copies[:3]:
        copy.wait()

    phase("pack")
    lists = lists_ref[...]
    user = iota((U, L), 0)
    count = jnp.zeros((U, L), I32)
    for u in range(U):
        count = jnp.where(user == u, counts_ref[u], count)
    live = iota((U, L), 1) < count
    block = lists >> 11
    holder = ((block >> 2) & 7) * NP + (block >> 5) * NY + (block & 3)
    local = lists & (ROWS - 1)
    holder = jnp.where(live, holder, -1)
    before = jnp.where((iota((L, 2 * L), 0) < iota((L, 2 * L), 1)) | (iota((L, 2 * L), 1) >= L), 1.0, 0.0).astype(BF16)
    base = jnp.zeros((NH, L), F32)
    ranks = []
    for u in range(U):
        hit = jnp.where(iota((NH, L), 0) == holder[u : u + 1, :], 1.0, 0.0)
        sums = dot(hit.astype(BF16), before)
        ranks.append(jnp.sum(hit * (sums[:, :L] + base), axis=0, keepdims=True))
        base = base + sums[:, L:]
    rank = jnp.concatenate(ranks, axis=0)
    place = jnp.where(live, holder.astype(F32) * CAP + rank, -1.0)
    place_t = jnp.concatenate([place, jnp.zeros((L - U, L), F32)], axis=0).T

    phase("weights")
    confidence = 1.0 + conf_scale * jnp.log(2.0 + plays_ref[...].astype(F32))
    full_weight = jnp.where(live, confidence, 0.0)
    full3 = [v.astype(F32) for v in pieces(full_weight)]
    id_hi = (local >> 4).astype(F32)
    id_lo = (local & 15).astype(F32)
    found = jnp.zeros((4 * U, NH * CAP), F32)
    for u in range(U):
        pick = jnp.where(place_t[:, u : u + 1] == iota((L, NH * CAP), 1).astype(F32), 1.0, 0.0).astype(BF16)
        names = jnp.where(user == 0, id_hi[u : u + 1, :], jnp.where(user == 1, id_lo[u : u + 1, :], 0.0))
        left = jnp.concatenate([jnp.where(user == u, v, 0.0) for v in full3] + [names], axis=0).astype(BF16)
        found = found + dot(left, pick)
    weight = folded(found, U)
    extra = jnp.where(weight > 0.0, weight - 1.0, 0.0)
    wanted = found[3 * U : 3 * U + 1] * 16.0 + found[3 * U + 1 : 3 * U + 2]
    for k in range(NZ):
        req_send[k] = wanted[:, k * L : (k + 1) * L]
    req_z[0] = req_send[z]

    phase("barrier")
    pl.semaphore_wait(barrier, NP * NR - 1 + NZ - 1)
    for dz in FAR_Z[:-1]:
        dev = z_device(dz)
        send(req_send.at[dev[1]], req_z.at[NZ - dz], req_sems.at[0], req_sems.at[1], dev)

    phase("gram")
    copies[4].wait()
    half = pl.ds(pl.multiple_of(r * (K // NR), K // NR), K // NR)
    part = lax.dot_general(items[:, half], items[...], (((0,), (0,)), ((), ())), preferred_element_type=F32)
    gram_mine[...] = part.reshape(NP, 8, K)
    gram_p[p] = gram_mine[p]
    phase("gram_p_send")
    for d in reversed(NEAR[1:]):
        dev = plane_device(d)
        send(gram_mine.at[place_of(dev)], gram_p.at[p], gram_sems.at[0], gram_sems.at[1], dev)

    phase("req_z_wait")
    wait_bytes(req_z.at[pl.ds(0, NZ - 1)], req_sems.at[1])
    req_fwd[...] = jnp.concatenate([req_z[...].reshape(NZ, L), jnp.zeros((L - NZ, L), F32)], axis=0).T.reshape(NP, CAP, L)
    phase("req_p_send")
    for k in reversed(range(1, NP)):
        dev = plane_device(NEAR[k])
        send(req_fwd.at[place_of(dev)], req_p.at[k], req_sems.at[2], req_recv.at[k], dev)

    phase("gram_p_wait")
    wait_bytes(gram_p.at[pl.ds(0, NP - 1)], gram_sems.at[1])
    gram_zsend[...] = jnp.sum(gram_p[...], axis=0)
    gram_z[z] = gram_zsend[...]
    for dz in FAR_Z[:-1]:
        send(gram_zsend, gram_z.at[z], gram_sems.at[2], gram_sems.at[3], z_device(dz))

    def serve(step):
        tiles = []
        for k in (2 * step, 2 * step + 1):
            if k:
                wait_bytes(req_p.at[k], req_recv.at[k])
            tiles.append(req_p[k] if k else req_fwd[p])
        column = jnp.concatenate([t[:, dz : dz + 1] for t in tiles for dz in FAR_Z], axis=0)
        total = jnp.zeros((2 * NZ * CAP, K), F32)
        width = 512
        for part in range(ROWS // width):
            pick = jnp.where(column == (iota((2 * NZ * CAP, width), 1) + part * width).astype(F32), 1.0, 0.0).astype(BF16)
            total = total + dot(pick, items[part * width : (part + 1) * width, :])
        rows_send[step] = total.reshape(2 * NZ, CAP, K).astype(BF16)
        send_rows(step, FAR_Z[:5])

    def send_rows(step, offsets):
        for dz in offsets:
            for i in (1, 0):
                d = NEAR[2 * step + i]
                dev = ((x - d[0]) & (NX - 1), (z + dz) & (NZ - 1), (y - d[1]) & (NY - 1), r)
                src = rows_send.at[step, i * NZ + FAR_Z.index(dz)]
                dst = rows_in.at[z * NP + p]
                if d == (0, 0) and dz == 0:
                    pltpu.make_async_copy(src, dst, rows_recv).start()
                else:
                    send(src, dst, rows_sem, rows_recv, dev)

    def spread_gram():
        wait_bytes(gram_z.at[pl.ds(0, NZ - 1)], gram_sems.at[3])
        gram_red[...] = jnp.sum(gram_z[...], axis=0)
        gram_full[r * NP + p] = gram_red[...]
        for d, same in peers:
            send(gram_red, gram_full.at[r * NP + p], gram_sems.at[4], gram_sems.at[5], plane_device(d, same))

    for n, step in enumerate(STEPS):
        phase("serve%d" % step)
        serve(step)
        if n == GRAM_AFTER:
            phase("gram_ag")
            spread_gram()
    phase("serve_near")
    for step in STEPS:
        send_rows(step, FAR_Z[5:7])
    for step in STEPS:
        send_rows(step, FAR_Z[7:])

    phase("gram_ag_wait")
    wait_bytes(gram_full.at[pl.ds(0, NP * NR - 1)], gram_sems.at[5])
    phase("gram_pieces")
    for k, piece in enumerate(pieces(gram_full[...].reshape(K, K))):
        gram3[:, k * K : (k + 1) * K] = piece

    phase("rows_wait")
    wait_bytes(rows_in, rows_recv)
    rows_mat[...] = rows_in[...].astype(F32).reshape(NH * CAP, K).astype(BF16)

    phase("cg")
    def image_of(v):
        v3 = stacked(v)
        along = folded(dot_nt(v3, rows_mat[...]), U)
        back = folded(dot(stacked(extra * along), rows_mat[...]), U)
        g = folded(dot(v3, gram3[...]), U)
        return g[:, :K] + g[:, K : 2 * K] + g[:, 2 * K :] + back + ridge * v

    def inner(a, b):
        return jnp.sum(a * b, axis=1, keepdims=True)

    target = folded(dot(stacked(weight), rows_mat[...]), U)
    copies[3].wait()
    solution = users_ref[...]
    residual = target - image_of(solution)
    direction = residual
    squares = inner(residual, residual)
    lane = iota((U, L), 1)
    collected = jnp.where(lane == 0, squares, 0.0)
    for t in range(ITERS):
        image = image_of(direction)
        alpha = squares / (inner(direction, image) + tiny)
        solution = solution + alpha * direction
        residual = residual - alpha * image
        fresh = inner(residual, residual)
        direction = residual + (fresh / (squares + tiny)) * direction
        squares = fresh
        collected = collected + jnp.where(lane == t + 1, squares, 0.0)

    norm_send[...] = jnp.sum(collected, axis=0, keepdims=True)
    phase("norm_pair")
    norm_pair[r] = norm_send[...]
    send(norm_send, norm_pair.at[r], norm_sems.at[0], norm_sems.at[1], plane_device((0, 0), 0))
    out_ref[...] = solution
    wait_bytes(req_z.at[pl.ds(0, NZ - 1)], req_sems.at[0])
    wait_bytes(req_p.at[pl.ds(0, NP - 1)], req_sems.at[2])
    wait_bytes(gram_mine.at[pl.ds(0, NP - 1)], gram_sems.at[0])
    wait_bytes(gram_z.at[pl.ds(0, NZ - 1)], gram_sems.at[2])
    wait_bytes(gram_full.at[pl.ds(0, NP * NR - 1)], gram_sems.at[4])
    wait_bytes(rows_in.at[pl.ds(0, NH - 1)], rows_sem)
    wait_bytes(norm_pair.at[pl.ds(0, 1)], norm_sems.at[1])
    norm_mid[...] = norm_pair[0] + norm_pair[1]
    phase("norm_all")
    norm_all[z * NP + p] = norm_mid[...]
    for d, dz in EVERY:
        dev = ((x + d[0]) & (NX - 1), (z + dz) & (NZ - 1), (y + d[1]) & (NY - 1), r)
        send(norm_mid, norm_all.at[z * NP + p], norm_sems.at[2], norm_sems.at[3], dev)
    wait_bytes(norm_pair.at[pl.ds(0, 1)], norm_sems.at[0])
    wait_bytes(norm_all.at[pl.ds(0, NH - 1)], norm_sems.at[3])
    phase("norm_end")
    total = jnp.sum(norm_all[...], axis=0)
    norms_ref[...] = jnp.sqrt(total / (USERS * K))[:, : ITERS + 1]
    wait_bytes(norm_all.at[pl.ds(0, NH - 1)], norm_sems.at[2])
    phase(None)


def body(item_factors, user_factors, item_lists, counts, plays):
    vmem = pl.BlockSpec(memory_space=pltpu.VMEM)
    dma = pltpu.SemaphoreType.DMA
    new_factors, norms = pl.pallas_call(
        kernel,
        out_shape=(pltpu.VMEM((U, K), F32), pltpu.VMEM((1, ITERS + 1), F32)),
        in_specs=[pl.BlockSpec(memory_space=pltpu.HBM)] * 5,
        out_specs=(vmem, vmem),
        scratch_shapes=[
            pltpu.SMEM((U,), I32),
            pltpu.VMEM((U, L), I32),
            pltpu.VMEM((U, L), I32),
            pltpu.VMEM((U, K), F32),
            pltpu.VMEM((ROWS, K), BF16),
            pltpu.VMEM((NZ, 1, L), F32),
            pltpu.VMEM((NZ, 1, L), F32),
            pltpu.VMEM((NP, CAP, L), F32),
            pltpu.VMEM((NP, CAP, L), F32),
            pltpu.VMEM((NP, 8, K), F32),
            pltpu.VMEM((NP, 8, K), F32),
            pltpu.VMEM((8, K), F32),
            pltpu.VMEM((NZ, 8, K), F32),
            pltpu.VMEM((8, K), F32),
            pltpu.VMEM((NR * NP, 8, K), F32),
            pltpu.VMEM((K, 3 * K), BF16),
            pltpu.VMEM((NP // 2, 2 * NZ, CAP, K), BF16),
            pltpu.VMEM((NH, CAP, K), BF16),
            pltpu.VMEM((NH * CAP, K), BF16),
            pltpu.VMEM((1, L), F32),
            pltpu.VMEM((NR, 1, L), F32),
            pltpu.VMEM((1, L), F32),
            pltpu.VMEM((NH, 1, L), F32),
            dma((5,)),
            dma((3,)),
            dma((NP,)),
            dma((6,)),
            dma,
            dma,
            dma((4,)),
        ],
        compiler_params=pltpu.CompilerParams(collective_id=0, has_side_effects=True),
    )(counts, item_lists, plays, user_factors, item_factors)
    return new_factors, norms.reshape(ITERS + 1)


def solution(mesh):
    split = Mesh(mesh.devices.reshape(NX, NZ, NY, NR), BLK_REP)
    in_specs = (P(BLK, None), P(BLK_REP, None), P(BLK_REP, None), P(BLK_REP), P(BLK_REP, None))
    out_specs = (P(BLK_REP, None), P())
    return jax.shard_map(body, mesh=split, in_specs=in_specs, out_specs=out_specs, check_vma=False)
```

```python
import jax
import jax.numpy as jnp
from jax import lax
from jax.experimental import pallas as pl
from jax.experimental.pallas import tpu as pltpu
from jax.sharding import Mesh
from jax.sharding import PartitionSpec as P

ITERS = 3
BLK_REP = ("blk_0", "blk_1", "blk_2", "rep")
BLK = ("blk_0", "blk_1", "blk_2")
MESH = pl.DeviceIdType.MESH

NX, NZ, NY, NR = 4, 8, 4, 2
NP = NX * NY
NH = NP * NZ
CAP = 8
U, L, K = 8, 128, 256
ROWS = 2048
USERS = U * NH * NR
EXCHANGE_AFTER, SPREAD_AFTER = 0, 5
F32, BF16, I32 = jnp.float32, jnp.bfloat16, jnp.int32

conf_scale = 40.0
ridge = 1.0
tiny = 1e-06


def dot(a, b):
    return jnp.dot(a, b, preferred_element_type=F32)


def dot_nt(a, b):
    return lax.dot_general(a, b, (((1,), (1,)), ((), ())), preferred_element_type=F32)


def pieces(v):
    hi = v.astype(BF16)
    rest = v - hi.astype(F32)
    mid = rest.astype(BF16)
    low = (rest - mid.astype(F32)).astype(BF16)
    return hi, mid, low


def stacked(v):
    hi, mid, low = pieces(v)
    return jnp.concatenate([hi.astype(F32), mid.astype(F32), low.astype(F32)], axis=0).astype(BF16)


def folded(v, n):
    return v[:n] + v[n : 2 * n] + v[2 * n : 3 * n]


def iota(shape, dim):
    return lax.broadcasted_iota(I32, shape, dim)


class Phases:
    def __init__(self):
        self.open = None

    def __call__(self, name):
        if self.open is not None:
            self.open.__exit__(None, None, None)
        self.open = jax.named_scope(name) if name else None
        if self.open is not None:
            self.open.__enter__()


NEAR = sorted(((dx, dy) for dx in range(NX) for dy in range(NY)), key=lambda d: (min(d[0], NX - d[0]) + min(d[1], NY - d[1]), d))
EVERY = sorted(
    ((d, dz) for d in NEAR for dz in range(NZ) if d != (0, 0) or dz),
    key=lambda o: -(min(o[0][0], NX - o[0][0]) + min(o[0][1], NY - o[0][1]) + min(o[1], NZ - o[1])),
)
TILES = (range(0,1),range(1,2),range(2,3),range(3,4),range(4,5), range(5,8), range(14,16), range(11, 14), range(8, 11))
FAR_Z = (4, 3, 5, 2, 6, 1, 7, 0)


def kernel(
    counts_hbm,
    lists_hbm,
    plays_hbm,
    users_hbm,
    items_hbm,
    out_ref,
    norms_ref,
    counts_ref,
    lists_ref,
    plays_ref,
    users_ref,
    items,
    req_send,
    req_z,
    req_fwd,
    req_p,
    gram_mine,
    gram_p,
    gram_zsend,
    gram_z,
    gram_red,
    gram_full,
    gram3,
    rows_send,
    rows_in,
    norm_send,
    norm_pair,
    norm_mid,
    norm_all,
    local_sems,
    req_sems,
    req_recv,
    gram_sems,
    rows_sem,
    rows_recv,
    norm_sems,
):
    phase = Phases()
    phase("enter")
    x, z, y, r = (lax.axis_index(a) for a in BLK_REP)
    p = x * NY + y

    def plane_device(d, same=1):
        return ((x + d[0]) & (NX - 1), z, (y + d[1]) & (NY - 1), r if same else 1 - r)

    def z_device(dz):
        return (x, (z + dz) & (NZ - 1), y, r)

    def place_of(dev):
        return dev[0] * NY + dev[2]

    peers = [(d, same) for same in (1, 0) for d in reversed(NEAR) if not (same and d == (0, 0))]

    def send(src, dst, send_sem, recv_sem, dev):
        pltpu.make_async_remote_copy(
            src_ref=src, dst_ref=dst, send_sem=send_sem, recv_sem=recv_sem, device_id=dev, device_id_type=MESH
        ).start()

    def wait_bytes(ref, sem):
        pltpu.make_async_copy(ref, ref, sem).wait()

    copies = [
        pltpu.make_async_copy(src, dst, local_sems.at[k])
        for k, (src, dst) in enumerate(
            [(counts_hbm, counts_ref), (lists_hbm, lists_ref), (plays_hbm, plays_ref), (users_hbm, users_ref), (items_hbm, items)]
        )
    ]
    for copy in copies:
        copy.start()
    barrier = pltpu.get_barrier_semaphore()
    for dz in range(1, NZ):
        pl.semaphore_signal(barrier, inc=1, device_id=z_device(dz), device_id_type=MESH)
    for d, same in peers:
        pl.semaphore_signal(barrier, inc=1, device_id=plane_device(d, same), device_id_type=MESH)
    for copy in copies[:3]:
        copy.wait()

    phase("pack")
    lists = lists_ref[...]
    user = iota((U, L), 0)
    count = jnp.zeros((U, L), I32)
    for u in range(U):
        count = jnp.where(user == u, counts_ref[u], count)
    live = iota((U, L), 1) < count
    block = lists >> 11
    holder = ((block >> 2) & 7) * NP + (block >> 5) * NY + (block & 3)
    local = lists & (ROWS - 1)
    holder = jnp.where(live, holder, -1)
    before = jnp.where((iota((L, 2 * L), 0) < iota((L, 2 * L), 1)) | (iota((L, 2 * L), 1) >= L), 1.0, 0.0).astype(BF16)
    base = jnp.zeros((NH, L), F32)
    ranks = []
    for u in range(U):
        hit = jnp.where(iota((NH, L), 0) == holder[u : u + 1, :], 1.0, 0.0)
        sums = dot(hit.astype(BF16), before)
        ranks.append(jnp.sum(hit * (sums[:, :L] + base), axis=0, keepdims=True))
        base = base + sums[:, L:]
    rank = jnp.concatenate(ranks, axis=0)
    place = jnp.where(live, holder.astype(F32) * CAP + rank, -1.0)
    place_t = jnp.concatenate([place, jnp.zeros((L - U, L), F32)], axis=0).T

    phase("weights")
    confidence = 1.0 + conf_scale * jnp.log(2.0 + plays_ref[...].astype(F32))
    full_weight = jnp.where(live, confidence, 0.0)
    full3 = [v.astype(F32) for v in pieces(full_weight)]
    id_hi = (local >> 4).astype(F32)
    id_lo = (local & 15).astype(F32)
    found = jnp.zeros((4 * U, NH * CAP), F32)
    for u in range(U):
        pick = jnp.where(place_t[:, u : u + 1] == iota((L, NH * CAP), 1).astype(F32), 1.0, 0.0).astype(BF16)
        names = jnp.where(user == 0, id_hi[u : u + 1, :], jnp.where(user == 1, id_lo[u : u + 1, :], 0.0))
        left = jnp.concatenate([jnp.where(user == u, v, 0.0) for v in full3] + [names], axis=0).astype(BF16)
        found = found + dot(left, pick)
    weight = folded(found, U)
    extra = jnp.where(weight > 0.0, weight - 1.0, 0.0)
    wanted = found[3 * U : 3 * U + 1] * 16.0 + found[3 * U + 1 : 3 * U + 2]
    for k in range(NZ):
        req_send[k] = wanted[:, k * L : (k + 1) * L]
    req_z[0] = req_send[z]

    phase("barrier")
    pl.semaphore_wait(barrier, NP * NR - 1 + NZ - 1)
    for dz in FAR_Z[:-1]:
        dev = z_device(dz)
        send(req_send.at[dev[1]], req_z.at[NZ - dz], req_sems.at[0], req_sems.at[1], dev)

    phase("gram")
    copies[4].wait()
    half = pl.ds(pl.multiple_of(r * (K // NR), K // NR), K // NR)
    part = lax.dot_general(items[:, half], items[...], (((0,), (0,)), ((), ())), preferred_element_type=F32)
    gram_mine[...] = part.reshape(NP, 8, K)
    gram_p[p] = gram_mine[p]
    phase("gram_p_send")
    for d in reversed(NEAR[1:]):
        dev = plane_device(d)
        send(gram_mine.at[place_of(dev)], gram_p.at[p], gram_sems.at[0], gram_sems.at[1], dev)

    phase("req_z_wait")
    wait_bytes(req_z.at[pl.ds(0, NZ - 1)], req_sems.at[1])
    req_fwd[...] = jnp.concatenate([req_z[...].reshape(NZ, L), jnp.zeros((L - NZ, L), F32)], axis=0).T.reshape(NP, CAP, L)
    phase("req_p_send")
    for k in reversed(range(1, NP)):
        dev = plane_device(NEAR[k])
        send(req_fwd.at[place_of(dev)], req_p.at[k], req_sems.at[2], req_recv.at[k], dev)

    def exchange_gram():
        wait_bytes(gram_p.at[pl.ds(0, NP - 1)], gram_sems.at[1])
        gram_zsend[...] = jnp.sum(gram_p[...], axis=0)
        gram_z[z] = gram_zsend[...]
        for dz in FAR_Z[:-1]:
            send(gram_zsend, gram_z.at[z], gram_sems.at[2], gram_sems.at[3], z_device(dz))

    def spread_gram():
        wait_bytes(gram_z.at[pl.ds(0, NZ - 1)], gram_sems.at[3])
        gram_red[...] = jnp.sum(gram_z[...], axis=0)
        gram_full[r * NP + p] = gram_red[...]
        for d, same in peers:
            send(gram_red, gram_full.at[r * NP + p], gram_sems.at[4], gram_sems.at[5], plane_device(d, same))

    def serve(tiles):
        for k in tiles:
            if k:
                wait_bytes(req_p.at[k], req_recv.at[k])
        asked = [req_p[k] if k else req_fwd[p] for k in tiles]
        column = jnp.concatenate([t[:, dz : dz + 1] for t in asked for dz in FAR_Z], axis=0)
        count = len(tiles) * NZ * CAP
        total = jnp.zeros((count, K), F32)
        width = 512
        for part in range(ROWS // width):
            pick = jnp.where(column == (iota((count, width), 1) + part * width).astype(F32), 1.0, 0.0).astype(BF16)
            total = total + dot(pick, items[part * width : (part + 1) * width, :])
        rows_send[tiles[0] * NZ : (tiles[-1] + 1) * NZ] = total.reshape(len(tiles) * NZ, CAP, K).astype(BF16)
        for j, dz in enumerate(FAR_Z):
            for k in reversed(tiles):
                d = NEAR[k]
                dev = ((x - d[0]) & (NX - 1), (z + dz) & (NZ - 1), (y - d[1]) & (NY - 1), r)
                src = rows_send.at[k * NZ + j]
                dst = rows_in.at[pl.ds(pl.multiple_of((z * NP + p) * CAP, CAP), CAP), :]
                if k == 0 and dz == 0:
                    pltpu.make_async_copy(src, dst, rows_recv).start()
                else:
                    send(src, dst, rows_sem, rows_recv, dev)

    for n, tiles in enumerate(TILES):
        phase("serve%d" % n)
        serve(tiles)
        if n == EXCHANGE_AFTER:
            phase("gram_z")
            exchange_gram()
        if n == SPREAD_AFTER:
            phase("gram_ag")
            spread_gram()

    phase("gram_ag_wait")
    wait_bytes(gram_full.at[pl.ds(0, NP * NR - 1)], gram_sems.at[5])
    phase("gram_pieces")
    for k, piece in enumerate(pieces(gram_full[...].reshape(K, K))):
        gram3[:, k * K : (k + 1) * K] = piece

    phase("rows_wait")
    wait_bytes(rows_in, rows_recv)

    phase("cg")
    def image_of(v):
        v3 = stacked(v)
        along = folded(dot_nt(v3, rows_in[...]), U)
        back = folded(dot(stacked(extra * along), rows_in[...]), U)
        g = folded(dot(v3, gram3[...]), U)
        return g[:, :K] + g[:, K : 2 * K] + g[:, 2 * K :] + back + ridge * v

    def inner(a, b):
        return jnp.sum(a * b, axis=1, keepdims=True)

    target = folded(dot(stacked(weight), rows_in[...]), U)
    copies[3].wait()
    solution = users_ref[...]
    residual = target - image_of(solution)
    direction = residual
    squares = inner(residual, residual)
    lane = iota((U, L), 1)
    collected = jnp.where(lane == 0, squares, 0.0)
    for t in range(ITERS):
        image = image_of(direction)
        alpha = squares / (inner(direction, image) + tiny)
        solution = solution + alpha * direction
        residual = residual - alpha * image
        fresh = inner(residual, residual)
        direction = residual + (fresh / (squares + tiny)) * direction
        squares = fresh
        collected = collected + jnp.where(lane == t + 1, squares, 0.0)

    norm_send[...] = jnp.sum(collected, axis=0, keepdims=True)
    phase("norm_pair")
    norm_pair[r] = norm_send[...]
    send(norm_send, norm_pair.at[r], norm_sems.at[0], norm_sems.at[1], plane_device((0, 0), 0))
    out_ref[...] = solution
    wait_bytes(req_z.at[pl.ds(0, NZ - 1)], req_sems.at[0])
    wait_bytes(req_p.at[pl.ds(0, NP - 1)], req_sems.at[2])
    wait_bytes(gram_mine.at[pl.ds(0, NP - 1)], gram_sems.at[0])
    wait_bytes(gram_z.at[pl.ds(0, NZ - 1)], gram_sems.at[2])
    wait_bytes(gram_full.at[pl.ds(0, NP * NR - 1)], gram_sems.at[4])
    wait_bytes(rows_send.at[pl.ds(0, NH - 1)], rows_sem)
    wait_bytes(norm_pair.at[pl.ds(0, 1)], norm_sems.at[1])
    norm_mid[...] = norm_pair[0] + norm_pair[1]
    phase("norm_all")
    norm_all[z * NP + p] = norm_mid[...]
    for d, dz in EVERY:
        dev = ((x + d[0]) & (NX - 1), (z + dz) & (NZ - 1), (y + d[1]) & (NY - 1), 1 - r)
        send(norm_mid, norm_all.at[z * NP + p], norm_sems.at[2], norm_sems.at[3], dev)
    wait_bytes(norm_pair.at[pl.ds(0, 1)], norm_sems.at[0])
    wait_bytes(norm_all.at[pl.ds(0, NH - 1)], norm_sems.at[3])
    phase("norm_end")
    total = jnp.sum(norm_all[...], axis=0)
    norms_ref[...] = jnp.sqrt(total / (USERS * K))[:, : ITERS + 1]
    wait_bytes(norm_all.at[pl.ds(0, NH - 1)], norm_sems.at[2])
    phase(None)


def body(item_factors, user_factors, item_lists, counts, plays):
    vmem = pl.BlockSpec(memory_space=pltpu.VMEM)
    dma = pltpu.SemaphoreType.DMA
    new_factors, norms = pl.pallas_call(
        kernel,
        out_shape=(pltpu.VMEM((U, K), F32), pltpu.VMEM((1, ITERS + 1), F32)),
        in_specs=[pl.BlockSpec(memory_space=pltpu.HBM)] * 5,
        out_specs=(vmem, vmem),
        scratch_shapes=[
            pltpu.SMEM((U,), I32),
            pltpu.VMEM((U, L), I32),
            pltpu.VMEM((U, L), I32),
            pltpu.VMEM((U, K), F32),
            pltpu.VMEM((ROWS, K), BF16),
            pltpu.VMEM((NZ, 1, L), F32),
            pltpu.VMEM((NZ, 1, L), F32),
            pltpu.VMEM((NP, CAP, L), F32),
            pltpu.VMEM((NP, CAP, L), F32),
            pltpu.VMEM((NP, 8, K), F32),
            pltpu.VMEM((NP, 8, K), F32),
            pltpu.VMEM((8, K), F32),
            pltpu.VMEM((NZ, 8, K), F32),
            pltpu.VMEM((8, K), F32),
            pltpu.VMEM((NR * NP, 8, K), F32),
            pltpu.VMEM((K, 3 * K), BF16),
            pltpu.VMEM((NP * NZ, CAP, K), BF16),
            pltpu.VMEM((NH * CAP, K), BF16),
            pltpu.VMEM((1, L), F32),
            pltpu.VMEM((NR, 1, L), F32),
            pltpu.VMEM((1, L), F32),
            pltpu.VMEM((NH, 1, L), F32),
            dma((5,)),
            dma((3,)),
            dma((NP,)),
            dma((6,)),
            dma,
            dma,
            dma((4,)),
        ],
        compiler_params=pltpu.CompilerParams(collective_id=0, has_side_effects=True),
    )(counts, item_lists, plays, user_factors, item_factors)
    return new_factors, norms.reshape(ITERS + 1)


def solution(mesh):
    split = Mesh(mesh.devices.reshape(NX, NZ, NY, NR), BLK_REP)
    in_specs = (P(BLK, None), P(BLK_REP, None), P(BLK_REP, None), P(BLK_REP), P(BLK_REP, None))
    out_specs = (P(BLK_REP, None), P())
    return jax.shard_map(body, mesh=split, in_specs=in_specs, out_specs=out_specs, check_vma=False)
```

```python
import jax
import jax.numpy as jnp
from jax import lax
from jax.experimental import pallas as pl
from jax.experimental.pallas import tpu as pltpu
from jax.sharding import Mesh
from jax.sharding import PartitionSpec as P

ITERS = 3
BLK_REP = ("blk_0", "blk_1", "blk_2", "rep")
BLK = ("blk_0", "blk_1", "blk_2")
MESH = pl.DeviceIdType.MESH

NX, NZ, NY, NR = 4, 8, 4, 2
NP = NX * NY
NH = NP * NZ
CAP = 8
U, L, K = 8, 128, 256
ROWS = 2048
USERS = U * NH * NR
EXCHANGE_AFTER, SPREAD_AFTER = 0, 5
F32, BF16, I32 = jnp.float32, jnp.bfloat16, jnp.int32

conf_scale = 40.0
ridge = 1.0
tiny = 1e-06


def dot(a, b):
    return jnp.dot(a, b, preferred_element_type=F32)


def dot_nt(a, b):
    return lax.dot_general(a, b, (((1,), (1,)), ((), ())), preferred_element_type=F32)


def pieces(v):
    hi = v.astype(BF16)
    rest = v - hi.astype(F32)
    mid = rest.astype(BF16)
    low = (rest - mid.astype(F32)).astype(BF16)
    return hi, mid, low


def stacked(v):
    hi, mid, low = pieces(v)
    return jnp.concatenate([hi.astype(F32), mid.astype(F32), low.astype(F32)], axis=0).astype(BF16)


def folded(v, n):
    return v[:n] + v[n : 2 * n] + v[2 * n : 3 * n]


def iota(shape, dim):
    return lax.broadcasted_iota(I32, shape, dim)


class Phases:
    def __init__(self):
        self.open = None

    def __call__(self, name):
        if self.open is not None:
            self.open.__exit__(None, None, None)
        self.open = jax.named_scope(name) if name else None
        if self.open is not None:
            self.open.__enter__()


NEAR = sorted(((dx, dy) for dx in range(NX) for dy in range(NY)), key=lambda d: (min(d[0], NX - d[0]) + min(d[1], NY - d[1]), d))
EVERY = sorted(
    ((d, dz) for d in NEAR for dz in range(NZ) if d != (0, 0) or dz),
    key=lambda o: -(min(o[0][0], NX - o[0][0]) + min(o[0][1], NY - o[0][1]) + min(o[1], NZ - o[1])),
)
TILES = (range(0,1),range(1,2),range(2,3),range(3,4),range(4,5), range(5,8), range(14,16), range(11, 14), range(8, 11))
FAR_Z = (4, 3, 5, 2, 6, 1, 7, 0)


def kernel(
    counts_hbm,
    lists_hbm,
    plays_hbm,
    users_hbm,
    items_hbm,
    out_ref,
    norms_ref,
    counts_ref,
    lists_ref,
    plays_ref,
    users_ref,
    items,
    req_send,
    req_z,
    req_fwd,
    req_p,
    gram_mine,
    gram_p,
    gram_zsend,
    gram_z,
    gram_red,
    gram_full,
    gram3,
    rows_send,
    rows_in,
    norm_send,
    norm_pair,
    norm_mid,
    norm_all,
    local_sems,
    req_sems,
    req_recv,
    gram_sems,
    rows_sem,
    rows_recv,
    norm_sems,
):
    phase = Phases()
    phase("enter")
    x, z, y, r = (lax.axis_index(a) for a in BLK_REP)
    p = x * NY + y

    def plane_device(d, same=1):
        return ((x + d[0]) & (NX - 1), z, (y + d[1]) & (NY - 1), r if same else 1 - r)

    def z_device(dz):
        return (x, (z + dz) & (NZ - 1), y, r)

    def place_of(dev):
        return dev[0] * NY + dev[2]

    peers = [(d, same) for same in (1, 0) for d in reversed(NEAR) if not (same and d == (0, 0))]

    def send(src, dst, send_sem, recv_sem, dev):
        pltpu.make_async_remote_copy(
            src_ref=src, dst_ref=dst, send_sem=send_sem, recv_sem=recv_sem, device_id=dev, device_id_type=MESH
        ).start()

    def wait_bytes(ref, sem):
        pltpu.make_async_copy(ref, ref, sem).wait()

    copies = [
        pltpu.make_async_copy(src, dst, local_sems.at[k])
        for k, (src, dst) in enumerate(
            [(counts_hbm, counts_ref), (lists_hbm, lists_ref), (plays_hbm, plays_ref), (users_hbm, users_ref), (items_hbm, items)]
        )
    ]
    for copy in copies:
        copy.start()
    barrier = pltpu.get_barrier_semaphore()
    for dz in range(1, NZ):
        pl.semaphore_signal(barrier, inc=1, device_id=z_device(dz), device_id_type=MESH)
    for d, same in peers:
        pl.semaphore_signal(barrier, inc=1, device_id=plane_device(d, same), device_id_type=MESH)
    for copy in copies[:3]:
        copy.wait()

    phase("pack")
    lists = lists_ref[...]
    user = iota((U, L), 0)
    count = jnp.zeros((U, L), I32)
    for u in range(U):
        count = jnp.where(user == u, counts_ref[u], count)
    live = iota((U, L), 1) < count
    block = lists >> 11
    holder = ((block >> 2) & 7) * NP + (block >> 5) * NY + (block & 3)
    local = lists & (ROWS - 1)
    holder = jnp.where(live, holder, -1)
    before = jnp.where((iota((L, 2 * L), 0) < iota((L, 2 * L), 1)) | (iota((L, 2 * L), 1) >= L), 1.0, 0.0).astype(BF16)
    base = jnp.zeros((NH, L), F32)
    ranks = []
    for u in range(U):
        hit = jnp.where(iota((NH, L), 0) == holder[u : u + 1, :], 1.0, 0.0)
        sums = dot(hit.astype(BF16), before)
        ranks.append(jnp.sum(hit * (sums[:, :L] + base), axis=0, keepdims=True))
        base = base + sums[:, L:]
    rank = jnp.concatenate(ranks, axis=0)
    place = jnp.where(live, holder.astype(F32) * CAP + rank, -1.0)
    place_t = jnp.concatenate([place, jnp.zeros((L - U, L), F32)], axis=0).T

    phase("weights")
    confidence = 1.0 + conf_scale * jnp.log(2.0 + plays_ref[...].astype(F32))
    full_weight = jnp.where(live, confidence, 0.0)
    full3 = [v.astype(F32) for v in pieces(full_weight)]
    id_hi = (local >> 4).astype(F32)
    id_lo = (local & 15).astype(F32)
    found = jnp.zeros((4 * U, NH * CAP), F32)
    for u in range(U):
        pick = jnp.where(place_t[:, u : u + 1] == iota((L, NH * CAP), 1).astype(F32), 1.0, 0.0).astype(BF16)
        names = jnp.where(user == 0, id_hi[u : u + 1, :], jnp.where(user == 1, id_lo[u : u + 1, :], 0.0))
        left = jnp.concatenate([jnp.where(user == u, v, 0.0) for v in full3] + [names], axis=0).astype(BF16)
        found = found + dot(left, pick)
    weight = folded(found, U)
    extra = jnp.where(weight > 0.0, weight - 1.0, 0.0)
    wanted = found[3 * U : 3 * U + 1] * 16.0 + found[3 * U + 1 : 3 * U + 2]
    for k in range(NZ):
        req_send[k] = wanted[:, k * L : (k + 1) * L]
    req_z[0] = req_send[z]

    phase("barrier")
    pl.semaphore_wait(barrier, NP * NR - 1 + NZ - 1)
    for dz in FAR_Z[:-1]:
        dev = z_device(dz)
        send(req_send.at[dev[1]], req_z.at[NZ - dz], req_sems.at[0], req_sems.at[1], dev)

    phase("gram")
    copies[4].wait()
    half = pl.ds(pl.multiple_of(r * (K // NR), K // NR), K // NR)
    part = lax.dot_general(items[:, half], items[...], (((0,), (0,)), ((), ())), preferred_element_type=F32)
    gram_mine[...] = part.reshape(NP, 8, K)
    gram_p[p] = gram_mine[p]
    phase("gram_p_send")
    for d in reversed(NEAR[1:]):
        dev = plane_device(d)
        send(gram_mine.at[place_of(dev)], gram_p.at[p], gram_sems.at[0], gram_sems.at[1], dev)

    phase("req_z_wait")
    wait_bytes(req_z.at[pl.ds(0, NZ - 1)], req_sems.at[1])
    req_fwd[...] = jnp.concatenate([req_z[...].reshape(NZ, L), jnp.zeros((L - NZ, L), F32)], axis=0).T.reshape(NP, CAP, L)
    phase("req_p_send")
    for k in reversed(range(1, NP)):
        dev = plane_device(NEAR[k])
        send(req_fwd.at[place_of(dev)], req_p.at[k], req_sems.at[2], req_recv.at[k], dev)

    def exchange_gram():
        wait_bytes(gram_p.at[pl.ds(0, NP - 1)], gram_sems.at[1])
        gram_zsend[...] = jnp.sum(gram_p[...], axis=0)
        gram_z[z] = gram_zsend[...]
        for dz in FAR_Z[:-1]:
            send(gram_zsend, gram_z.at[z], gram_sems.at[2], gram_sems.at[3], z_device(dz))

    def spread_gram():
        wait_bytes(gram_z.at[pl.ds(0, NZ - 1)], gram_sems.at[3])
        gram_red[...] = jnp.sum(gram_z[...], axis=0)
        gram_full[r * NP + p] = gram_red[...]
        for d, same in peers:
            send(gram_red, gram_full.at[r * NP + p], gram_sems.at[4], gram_sems.at[5], plane_device(d, same))

    def serve(tiles):
        for k in tiles:
            if k:
                wait_bytes(req_p.at[k], req_recv.at[k])
        asked = [req_p[k] if k else req_fwd[p] for k in tiles]
        column = jnp.concatenate([t[:, dz : dz + 1] for t in asked for dz in FAR_Z], axis=0)
        count = len(tiles) * NZ * CAP
        total = jnp.zeros((count, K), F32)
        width = 512
        for part in range(ROWS // width):
            pick = jnp.where(column == (iota((count, width), 1) + part * width).astype(F32), 1.0, 0.0).astype(BF16)
            total = total + dot(pick, items[part * width : (part + 1) * width, :])
        rows_send[tiles[0] * NZ : (tiles[-1] + 1) * NZ] = total.reshape(len(tiles) * NZ, CAP, K).astype(BF16)
        for j, dz in enumerate(FAR_Z):
            for k in reversed(tiles):
                d = NEAR[k]
                dev = ((x - d[0]) & (NX - 1), (z + dz) & (NZ - 1), (y - d[1]) & (NY - 1), r)
                src = rows_send.at[k * NZ + j]
                dst = rows_in.at[pl.ds(pl.multiple_of((z * NP + p) * CAP, CAP), CAP), :]
                if k == 0 and dz == 0:
                    pltpu.make_async_copy(src, dst, rows_recv).start()
                else:
                    send(src, dst, rows_sem, rows_recv, dev)

    for n, tiles in enumerate(TILES):
        phase("serve%d" % n)
        serve(tiles)
        if n == EXCHANGE_AFTER:
            phase("gram_z")
            exchange_gram()
        if n == SPREAD_AFTER:
            phase("gram_ag")
            spread_gram()

    phase("gram_ag_wait")
    wait_bytes(gram_full.at[pl.ds(0, NP * NR - 1)], gram_sems.at[5])
    phase("gram_pieces")
    for k, piece in enumerate(pieces(gram_full[...].reshape(K, K))):
        gram3[:, k * K : (k + 1) * K] = piece

    def gram_part(v3):
        g = folded(dot(v3, gram3[...]), U)
        return g[:, :K] + g[:, K : 2 * K] + g[:, 2 * K :]

    copies[3].wait()
    start = users_ref[...]
    start3 = stacked(start)
    start_image = gram_part(start3) + ridge * start
    weight3 = stacked(weight)

    phase("rows_wait")
    wait_bytes(rows_in, rows_recv)

    phase("cg")
    def image_of(v):
        v3 = stacked(v)
        along = folded(dot_nt(v3, rows_in[...]), U)
        back = folded(dot(stacked(extra * along), rows_in[...]), U)
        return gram_part(v3) + back + ridge * v

    def inner(a, b):
        return jnp.sum(a * b, axis=1, keepdims=True)

    along = folded(dot_nt(start3, rows_in[...]), U)
    both = dot(jnp.concatenate([weight3.astype(F32), stacked(extra * along).astype(F32)], axis=0).astype(BF16), rows_in[...])
    solution = start
    residual = folded(both[: 3 * U], U) - (start_image + folded(both[3 * U :], U))
    direction = residual
    squares = inner(residual, residual)
    lane = iota((U, L), 1)
    collected = jnp.where(lane == 0, squares, 0.0)
    for t in range(ITERS):
        image = image_of(direction)
        alpha = squares / (inner(direction, image) + tiny)
        solution = solution + alpha * direction
        residual = residual - alpha * image
        fresh = inner(residual, residual)
        direction = residual + (fresh / (squares + tiny)) * direction
        squares = fresh
        collected = collected + jnp.where(lane == t + 1, squares, 0.0)

    norm_send[...] = jnp.sum(collected, axis=0, keepdims=True)
    phase("norm_pair")
    norm_pair[r] = norm_send[...]
    send(norm_send, norm_pair.at[r], norm_sems.at[0], norm_sems.at[1], plane_device((0, 0), 0))
    out_ref[...] = solution
    wait_bytes(req_z.at[pl.ds(0, NZ - 1)], req_sems.at[0])
    wait_bytes(req_p.at[pl.ds(0, NP - 1)], req_sems.at[2])
    wait_bytes(gram_mine.at[pl.ds(0, NP - 1)], gram_sems.at[0])
    wait_bytes(gram_z.at[pl.ds(0, NZ - 1)], gram_sems.at[2])
    wait_bytes(gram_full.at[pl.ds(0, NP * NR - 1)], gram_sems.at[4])
    wait_bytes(rows_send.at[pl.ds(0, NH - 1)], rows_sem)
    wait_bytes(norm_pair.at[pl.ds(0, 1)], norm_sems.at[1])
    norm_mid[...] = norm_pair[0] + norm_pair[1]
    phase("norm_all")
    norm_all[z * NP + p] = norm_mid[...]
    for d, dz in EVERY:
        dev = ((x + d[0]) & (NX - 1), (z + dz) & (NZ - 1), (y + d[1]) & (NY - 1), 1 - r)
        send(norm_mid, norm_all.at[z * NP + p], norm_sems.at[2], norm_sems.at[3], dev)
    wait_bytes(norm_pair.at[pl.ds(0, 1)], norm_sems.at[0])
    wait_bytes(norm_all.at[pl.ds(0, NH - 1)], norm_sems.at[3])
    phase("norm_end")
    total = jnp.sum(norm_all[...], axis=0)
    norms_ref[...] = jnp.sqrt(total / (USERS * K))[:, : ITERS + 1]
    wait_bytes(norm_all.at[pl.ds(0, NH - 1)], norm_sems.at[2])
    phase(None)


def put_out(factors, norms, factors_out, norms_out, sems):
    copies = [pltpu.make_async_copy(factors, factors_out, sems.at[0]), pltpu.make_async_copy(norms, norms_out, sems.at[1])]
    for copy in copies:
        copy.start()
    for copy in copies:
        copy.wait()


def body(item_factors, user_factors, item_lists, counts, plays):
    vmem = pl.BlockSpec(memory_space=pltpu.VMEM)
    dma = pltpu.SemaphoreType.DMA
    new_factors, norms = pl.pallas_call(
        kernel,
        out_shape=(pltpu.VMEM((U, K), F32), pltpu.VMEM((1, ITERS + 1), F32)),
        in_specs=[pl.BlockSpec(memory_space=pltpu.HBM)] * 5,
        out_specs=(vmem, vmem),
        scratch_shapes=[
            pltpu.SMEM((U,), I32),
            pltpu.VMEM((U, L), I32),
            pltpu.VMEM((U, L), I32),
            pltpu.VMEM((U, K), F32),
            pltpu.VMEM((ROWS, K), BF16),
            pltpu.VMEM((NZ, 1, L), F32),
            pltpu.VMEM((NZ, 1, L), F32),
            pltpu.VMEM((NP, CAP, L), F32),
            pltpu.VMEM((NP, CAP, L), F32),
            pltpu.VMEM((NP, 8, K), F32),
            pltpu.VMEM((NP, 8, K), F32),
            pltpu.VMEM((8, K), F32),
            pltpu.VMEM((NZ, 8, K), F32),
            pltpu.VMEM((8, K), F32),
            pltpu.VMEM((NR * NP, 8, K), F32),
            pltpu.VMEM((K, 3 * K), BF16),
            pltpu.VMEM((NP * NZ, CAP, K), BF16),
            pltpu.VMEM((NH * CAP, K), BF16),
            pltpu.VMEM((1, L), F32),
            pltpu.VMEM((NR, 1, L), F32),
            pltpu.VMEM((1, L), F32),
            pltpu.VMEM((NH, 1, L), F32),
            dma((5,)),
            dma((3,)),
            dma((NP,)),
            dma((6,)),
            dma,
            dma,
            dma((4,)),
        ],
        compiler_params=pltpu.CompilerParams(collective_id=0, has_side_effects=True),
    )(counts, item_lists, plays, user_factors, item_factors)
    new_factors, norms = pl.pallas_call(
        put_out,
        out_shape=(jax.ShapeDtypeStruct((U, K), F32), jax.ShapeDtypeStruct((1, ITERS + 1), F32)),
        in_specs=[vmem, vmem],
        out_specs=(pl.BlockSpec(memory_space=pltpu.HBM), pl.BlockSpec(memory_space=pltpu.HBM)),
        scratch_shapes=[dma((2,))],
        compiler_params=pltpu.CompilerParams(vmem_limit_bytes=1024 * 1024),
    )(new_factors, norms)
    return new_factors, norms.reshape(ITERS + 1)


def solution(mesh):
    split = Mesh(mesh.devices.reshape(NX, NZ, NY, NR), BLK_REP)
    in_specs = (P(BLK, None), P(BLK_REP, None), P(BLK_REP, None), P(BLK_REP), P(BLK_REP, None))
    out_specs = (P(BLK_REP, None), P())
    return jax.shard_map(body, mesh=split, in_specs=in_specs, out_specs=out_specs, check_vma=False)
```

```python
import jax
import jax.numpy as jnp
from jax import lax
from jax.experimental import pallas as pl
from jax.experimental.pallas import tpu as pltpu
from jax.sharding import Mesh
from jax.sharding import PartitionSpec as P

ITERS = 3
BLK_REP = ("blk_0", "blk_1", "blk_2", "rep")
BLK = ("blk_0", "blk_1", "blk_2")
MESH = pl.DeviceIdType.MESH

NX, NZ, NY, NR = 4, 8, 4, 2
NP = NX * NY
NH = NP * NZ
CAP = 8
U, L, K = 8, 128, 256
ROWS = 2048
USERS = U * NH * NR
EXCHANGE_AFTER, SPREAD_AFTER = 0, 4
F32, BF16, I32 = jnp.float32, jnp.bfloat16, jnp.int32

conf_scale = 40.0
ridge = 1.0
tiny = 1e-06


def dot(a, b):
    return jnp.dot(a, b, preferred_element_type=F32)


def dot_nt(a, b):
    return lax.dot_general(a, b, (((1,), (1,)), ((), ())), preferred_element_type=F32)


def pieces(v):
    hi = v.astype(BF16)
    rest = v - hi.astype(F32)
    mid = rest.astype(BF16)
    low = (rest - mid.astype(F32)).astype(BF16)
    return hi, mid, low


def stacked(v):
    hi, mid, low = pieces(v)
    return jnp.concatenate([hi.astype(F32), mid.astype(F32), low.astype(F32)], axis=0).astype(BF16)


def folded(v, n):
    return v[:n] + v[n : 2 * n] + v[2 * n : 3 * n]


def iota(shape, dim):
    return lax.broadcasted_iota(I32, shape, dim)


class Phases:
    def __init__(self):
        self.open = None

    def __call__(self, name):
        if self.open is not None:
            self.open.__exit__(None, None, None)
        self.open = jax.named_scope(name) if name else None
        if self.open is not None:
            self.open.__enter__()


NEAR = sorted(((dx, dy) for dx in range(NX) for dy in range(NY)), key=lambda d: (min(d[0], NX - d[0]) + min(d[1], NY - d[1]), d))
EVERY = sorted(
    ((d, dz) for d in NEAR for dz in range(NZ) if d != (0, 0) or dz),
    key=lambda o: -(min(o[0][0], NX - o[0][0]) + min(o[0][1], NY - o[0][1]) + min(o[1], NZ - o[1])),
)
DIRECT = range(1, 5)
DIRECT_Z = (3, 5, 2, 6, 1, 7, 0)
GROUPS = (
    [(0, dz) for dz in (4, 3, 5, 2, 6, 1, 7, 0)],
    [(k, dz) for dz in DIRECT_Z for k in DIRECT],
    *([(k, dz) for dz in (4, 3, 5, 2, 6, 1, 7, 0) for k in (*more, *tiles) if dz == 4 or k in tiles]
      for tiles, more in ((range(5, 8), DIRECT), (range(14, 16), ()), (range(11, 14), ()), (range(8, 11), ()))),
)
FAR_Z = (4, 3, 5, 2, 6, 1, 7, 0)


def hops(d, dz):
    return min(d[0], NX - d[0]) + min(d[1], NY - d[1]) + min(dz, NZ - dz)


def direct_slot(k, dz):
    return (k - DIRECT[0]) * len(DIRECT_Z) + DIRECT_Z.index(dz)


def kernel(
    counts_hbm,
    lists_hbm,
    plays_hbm,
    users_hbm,
    items_hbm,
    out_ref,
    norms_ref,
    counts_ref,
    lists_ref,
    plays_ref,
    users_ref,
    items,
    req_send,
    req_z,
    req_near,
    req_near_t,
    req_fwd,
    req_p,
    gram_mine,
    gram_p,
    gram_zsend,
    gram_z,
    gram_red,
    gram_full,
    gram3,
    rows_send,
    rows_in,
    norm_send,
    norm_pair,
    norm_mid,
    norm_all,
    local_sems,
    req_sems,
    req_near_recv,
    req_recv,
    gram_sems,
    rows_sem,
    rows_recv,
    norm_sems,
):
    phase = Phases()
    phase("enter")
    x, z, y, r = (lax.axis_index(a) for a in BLK_REP)
    p = x * NY + y

    def plane_device(d, same=1):
        return ((x + d[0]) & (NX - 1), z, (y + d[1]) & (NY - 1), r if same else 1 - r)

    def device(d, dz):
        return ((x + d[0]) & (NX - 1), (z + dz) & (NZ - 1), (y + d[1]) & (NY - 1), r)

    def z_device(dz):
        return (x, (z + dz) & (NZ - 1), y, r)

    def place_of(dev):
        return dev[0] * NY + dev[2]

    peers = [(d, same) for same in (1, 0) for d in reversed(NEAR) if not (same and d == (0, 0))]

    def send(src, dst, send_sem, recv_sem, dev):
        pltpu.make_async_remote_copy(
            src_ref=src, dst_ref=dst, send_sem=send_sem, recv_sem=recv_sem, device_id=dev, device_id_type=MESH
        ).start()

    def wait_bytes(ref, sem):
        pltpu.make_async_copy(ref, ref, sem).wait()

    copies = [
        pltpu.make_async_copy(src, dst, local_sems.at[k])
        for k, (src, dst) in enumerate(
            [(counts_hbm, counts_ref), (lists_hbm, lists_ref), (plays_hbm, plays_ref), (users_hbm, users_ref), (items_hbm, items)]
        )
    ]
    for copy in copies:
        copy.start()
    barrier = pltpu.get_barrier_semaphore()
    greeted = [((0, 0), dz, 1) for dz in range(1, NZ)] + [(d, 0, same) for d, same in peers]
    greeted += [(NEAR[k], dz, 1) for k in DIRECT for dz in DIRECT_Z[:-1]]
    for d, dz, same in sorted(greeted, key=lambda o: -hops(o[0], o[1])):
        dev = (*device(d, dz)[:3], r if same else 1 - r)
        pl.semaphore_signal(barrier, inc=1, device_id=dev, device_id_type=MESH)
    for copy in copies[:3]:
        copy.wait()

    phase("pack")
    lists = lists_ref[...]
    user = iota((U, L), 0)
    count = jnp.zeros((U, L), I32)
    for u in range(U):
        count = jnp.where(user == u, counts_ref[u], count)
    live = iota((U, L), 1) < count
    block = lists >> 11
    holder = ((block >> 2) & 7) * NP + (block >> 5) * NY + (block & 3)
    local = lists & (ROWS - 1)
    holder = jnp.where(live, holder, -1)
    before = jnp.where((iota((L, 2 * L), 0) < iota((L, 2 * L), 1)) | (iota((L, 2 * L), 1) >= L), 1.0, 0.0).astype(BF16)
    base = jnp.zeros((NH, L), F32)
    ranks = []
    for u in range(U):
        hit = jnp.where(iota((NH, L), 0) == holder[u : u + 1, :], 1.0, 0.0)
        sums = dot(hit.astype(BF16), before)
        ranks.append(jnp.sum(hit * (sums[:, :L] + base), axis=0, keepdims=True))
        base = base + sums[:, L:]
    rank = jnp.concatenate(ranks, axis=0)
    place = jnp.where(live, holder.astype(F32) * CAP + rank, -1.0)
    place_t = jnp.concatenate([place, jnp.zeros((L - U, L), F32)], axis=0).T

    phase("weights")
    confidence = 1.0 + conf_scale * jnp.log(2.0 + plays_ref[...].astype(F32))
    full_weight = jnp.where(live, confidence, 0.0)
    full3 = [v.astype(F32) for v in pieces(full_weight)]
    id_hi = (local >> 4).astype(F32)
    id_lo = (local & 15).astype(F32)
    found = jnp.zeros((4 * U, NH * CAP), F32)
    for u in range(U):
        pick = jnp.where(place_t[:, u : u + 1] == iota((L, NH * CAP), 1).astype(F32), 1.0, 0.0).astype(BF16)
        names = jnp.where(user == 0, id_hi[u : u + 1, :], jnp.where(user == 1, id_lo[u : u + 1, :], 0.0))
        left = jnp.concatenate([jnp.where(user == u, v, 0.0) for v in full3] + [names], axis=0).astype(BF16)
        found = found + dot(left, pick)
    weight = folded(found, U)
    extra = jnp.where(weight > 0.0, weight - 1.0, 0.0)
    wanted = found[3 * U : 3 * U + 1] * 16.0 + found[3 * U + 1 : 3 * U + 2]
    for k in range(NZ):
        req_send[k] = wanted[:, k * L : (k + 1) * L]
    req_z[0] = req_send[z]

    phase("barrier")
    pl.semaphore_wait(barrier, len(greeted))
    for dz in FAR_Z[:-1]:
        dev = z_device(dz)
        send(req_send.at[dev[1]], req_z.at[NZ - dz], req_sems.at[0], req_sems.at[1], dev)
    for dz in DIRECT_Z:
        for k in DIRECT:
            dev = device(NEAR[k], dz)
            at = direct_slot(k, (NZ - dz) % NZ)
            send(req_send.at[dev[1]], req_near.at[at], req_sems.at[0], req_near_recv, dev)

    phase("gram")
    copies[4].wait()
    half = pl.ds(pl.multiple_of(r * (K // NR), K // NR), K // NR)
    part = lax.dot_general(items[:, half], items[...], (((0,), (0,)), ((), ())), preferred_element_type=F32)
    gram_mine[...] = part.reshape(NP, 8, K)
    gram_p[p] = gram_mine[p]
    phase("gram_p_send")
    for d in reversed(NEAR[1:]):
        dev = plane_device(d)
        send(gram_mine.at[place_of(dev)], gram_p.at[p], gram_sems.at[0], gram_sems.at[1], dev)

    phase("req_z_wait")
    wait_bytes(req_z.at[pl.ds(0, NZ - 1)], req_sems.at[1])
    req_fwd[...] = jnp.concatenate([req_z[...].reshape(NZ, L), jnp.zeros((L - NZ, L), F32)], axis=0).T.reshape(NP, CAP, L)
    phase("req_p_send")
    for k in reversed(range(1, NP)):
        dev = plane_device(NEAR[k])
        send(req_fwd.at[place_of(dev)], req_p.at[k], req_sems.at[2], req_recv.at[k], dev)

    def exchange_gram():
        wait_bytes(gram_p.at[pl.ds(0, NP - 1)], gram_sems.at[1])
        gram_zsend[...] = jnp.sum(gram_p[...], axis=0)
        gram_z[z] = gram_zsend[...]
        for dz in FAR_Z[:-1]:
            send(gram_zsend, gram_z.at[z], gram_sems.at[2], gram_sems.at[3], z_device(dz))

    def spread_gram():
        wait_bytes(gram_z.at[pl.ds(0, NZ - 1)], gram_sems.at[3])
        gram_red[...] = jnp.sum(gram_z[...], axis=0)
        gram_full[r * NP + p] = gram_red[...]
        for d, same in peers:
            send(gram_red, gram_full.at[r * NP + p], gram_sems.at[4], gram_sems.at[5], plane_device(d, same))

    def serve(first, goals):
        direct = goals is GROUPS[1]
        if direct:
            wait_bytes(req_near, req_near_recv)
            known = len(DIRECT) * len(DIRECT_Z)
            near = jnp.concatenate([req_near[...].reshape(known, L), jnp.zeros((L - known, L), F32)], axis=0).T
            req_near_t[...] = near.reshape(NP, CAP, L)
            near = req_near_t[p]
            columns = [near[:, direct_slot(k, dz) : direct_slot(k, dz) + 1] for k, dz in goals]
        else:
            tiles = {}
            for k in sorted({k for k, _ in goals}):
                if k:
                    wait_bytes(req_p.at[k], req_recv.at[k])
                tiles[k] = req_p[k] if k else req_fwd[p]
            columns = [tiles[k][:, dz : dz + 1] for k, dz in goals]
        column = jnp.concatenate(columns, axis=0)
        count = len(goals) * CAP
        total = jnp.zeros((count, K), F32)
        width = 512
        for part in range(ROWS // width):
            pick = jnp.where(column == (iota((count, width), 1) + part * width).astype(F32), 1.0, 0.0).astype(BF16)
            total = total + dot(pick, items[part * width : (part + 1) * width, :])
        rows_send[first : first + len(goals)] = total.reshape(len(goals), CAP, K).astype(BF16)
        for i, (k, dz) in enumerate(goals):
            d = NEAR[k]
            dev = ((x - d[0]) & (NX - 1), (z + dz) & (NZ - 1), (y - d[1]) & (NY - 1), r)
            src = rows_send.at[first + i]
            dst = rows_in.at[pl.ds(pl.multiple_of((z * NP + p) * CAP, CAP), CAP), :]
            if k == 0 and dz == 0:
                pltpu.make_async_copy(src, dst, rows_recv).start()
            else:
                send(src, dst, rows_sem, rows_recv, dev)
        return first + len(goals)

    served = 0
    for n, goals in enumerate(GROUPS):
        phase("serve%d" % n)
        served = serve(served, goals)
        if n == EXCHANGE_AFTER:
            phase("gram_z")
            exchange_gram()
        if n == SPREAD_AFTER:
            phase("gram_ag")
            spread_gram()

    phase("gram_ag_wait")
    wait_bytes(gram_full.at[pl.ds(0, NP * NR - 1)], gram_sems.at[5])
    phase("gram_pieces")
    for k, piece in enumerate(pieces(gram_full[...].reshape(K, K))):
        gram3[:, k * K : (k + 1) * K] = piece

    def gram_part(v3):
        g = folded(dot(v3, gram3[...]), U)
        return g[:, :K] + g[:, K : 2 * K] + g[:, 2 * K :]

    copies[3].wait()
    start = users_ref[...]
    start3 = stacked(start)
    start_image = gram_part(start3) + ridge * start
    weight3 = stacked(weight)

    phase("rows_wait")
    wait_bytes(rows_in, rows_recv)

    phase("cg")
    def image_of(v):
        v3 = stacked(v)
        along = folded(dot_nt(v3, rows_in[...]), U)
        back = folded(dot(stacked(extra * along), rows_in[...]), U)
        return gram_part(v3) + back + ridge * v

    def inner(a, b):
        return jnp.sum(a * b, axis=1, keepdims=True)

    along = folded(dot_nt(start3, rows_in[...]), U)
    both = dot(jnp.concatenate([weight3.astype(F32), stacked(extra * along).astype(F32)], axis=0).astype(BF16), rows_in[...])
    solution = start
    residual = folded(both[: 3 * U], U) - (start_image + folded(both[3 * U :], U))
    direction = residual
    squares = inner(residual, residual)
    lane = iota((U, L), 1)
    collected = jnp.where(lane == 0, squares, 0.0)
    for t in range(ITERS):
        image = image_of(direction)
        alpha = squares / (inner(direction, image) + tiny)
        solution = solution + alpha * direction
        residual = residual - alpha * image
        fresh = inner(residual, residual)
        direction = residual + (fresh / (squares + tiny)) * direction
        squares = fresh
        collected = collected + jnp.where(lane == t + 1, squares, 0.0)

    norm_send[...] = jnp.sum(collected, axis=0, keepdims=True)
    phase("norm_pair")
    norm_pair[r] = norm_send[...]
    send(norm_send, norm_pair.at[r], norm_sems.at[0], norm_sems.at[1], plane_device((0, 0), 0))
    out_ref[...] = solution
    wait_bytes(req_z.at[pl.ds(0, NZ - 1)], req_sems.at[0])
    wait_bytes(req_near, req_sems.at[0])
    wait_bytes(req_p.at[pl.ds(0, NP - 1)], req_sems.at[2])
    wait_bytes(gram_mine.at[pl.ds(0, NP - 1)], gram_sems.at[0])
    wait_bytes(gram_z.at[pl.ds(0, NZ - 1)], gram_sems.at[2])
    wait_bytes(gram_full.at[pl.ds(0, NP * NR - 1)], gram_sems.at[4])
    wait_bytes(rows_send.at[pl.ds(0, NH - 1)], rows_sem)
    wait_bytes(norm_pair.at[pl.ds(0, 1)], norm_sems.at[1])
    norm_mid[...] = norm_pair[0] + norm_pair[1]
    phase("norm_all")
    norm_all[z * NP + p] = norm_mid[...]
    for d, dz in EVERY:
        dev = ((x + d[0]) & (NX - 1), (z + dz) & (NZ - 1), (y + d[1]) & (NY - 1), 1 - r)
        send(norm_mid, norm_all.at[z * NP + p], norm_sems.at[2], norm_sems.at[3], dev)
    wait_bytes(norm_pair.at[pl.ds(0, 1)], norm_sems.at[0])
    wait_bytes(norm_all.at[pl.ds(0, NH - 1)], norm_sems.at[3])
    phase("norm_end")
    total = jnp.sum(norm_all[...], axis=0)
    norms_ref[...] = jnp.sqrt(total / (USERS * K))[:, : ITERS + 1]
    wait_bytes(norm_all.at[pl.ds(0, NH - 1)], norm_sems.at[2])
    phase(None)


def put_out(factors, norms, factors_out, norms_out, sems):
    copies = [pltpu.make_async_copy(factors, factors_out, sems.at[0]), pltpu.make_async_copy(norms, norms_out, sems.at[1])]
    for copy in copies:
        copy.start()
    for copy in copies:
        copy.wait()


def body(item_factors, user_factors, item_lists, counts, plays):
    vmem = pl.BlockSpec(memory_space=pltpu.VMEM)
    dma = pltpu.SemaphoreType.DMA
    new_factors, norms = pl.pallas_call(
        kernel,
        out_shape=(pltpu.VMEM((U, K), F32), pltpu.VMEM((1, ITERS + 1), F32)),
        in_specs=[pl.BlockSpec(memory_space=pltpu.HBM)] * 5,
        out_specs=(vmem, vmem),
        scratch_shapes=[
            pltpu.SMEM((U,), I32),
            pltpu.VMEM((U, L), I32),
            pltpu.VMEM((U, L), I32),
            pltpu.VMEM((U, K), F32),
            pltpu.VMEM((ROWS, K), BF16),
            pltpu.VMEM((NZ, 1, L), F32),
            pltpu.VMEM((NZ, 1, L), F32),
            pltpu.VMEM((len(DIRECT) * len(DIRECT_Z), 1, L), F32),
            pltpu.VMEM((NP, CAP, L), F32),
            pltpu.VMEM((NP, CAP, L), F32),
            pltpu.VMEM((NP, CAP, L), F32),
            pltpu.VMEM((NP, 8, K), F32),
            pltpu.VMEM((NP, 8, K), F32),
            pltpu.VMEM((8, K), F32),
            pltpu.VMEM((NZ, 8, K), F32),
            pltpu.VMEM((8, K), F32),
            pltpu.VMEM((NR * NP, 8, K), F32),
            pltpu.VMEM((K, 3 * K), BF16),
            pltpu.VMEM((NP * NZ, CAP, K), BF16),
            pltpu.VMEM((NH * CAP, K), BF16),
            pltpu.VMEM((1, L), F32),
            pltpu.VMEM((NR, 1, L), F32),
            pltpu.VMEM((1, L), F32),
            pltpu.VMEM((NH, 1, L), F32),
            dma((5,)),
            dma((3,)),
            dma,
            dma((NP,)),
            dma((6,)),
            dma,
            dma,
            dma((4,)),
        ],
        compiler_params=pltpu.CompilerParams(collective_id=0, has_side_effects=True),
    )(counts, item_lists, plays, user_factors, item_factors)
    new_factors, norms = pl.pallas_call(
        put_out,
        out_shape=(jax.ShapeDtypeStruct((U, K), F32), jax.ShapeDtypeStruct((1, ITERS + 1), F32)),
        in_specs=[vmem, vmem],
        out_specs=(pl.BlockSpec(memory_space=pltpu.HBM), pl.BlockSpec(memory_space=pltpu.HBM)),
        scratch_shapes=[dma((2,))],
        compiler_params=pltpu.CompilerParams(vmem_limit_bytes=1024 * 1024),
    )(new_factors, norms)
    return new_factors, norms.reshape(ITERS + 1)


def solution(mesh):
    split = Mesh(mesh.devices.reshape(NX, NZ, NY, NR), BLK_REP)
    in_specs = (P(BLK, None), P(BLK_REP, None), P(BLK_REP, None), P(BLK_REP), P(BLK_REP, None))
    out_specs = (P(BLK_REP, None), P())
    return jax.shard_map(body, mesh=split, in_specs=in_specs, out_specs=out_specs, check_vma=False)
```

```python
import jax
import jax.numpy as jnp
from jax import lax
from jax.experimental import pallas as pl
from jax.experimental.pallas import tpu as pltpu
from jax.sharding import Mesh
from jax.sharding import PartitionSpec as P

ITERS = 3
BLK_REP = ("blk_0", "blk_1", "blk_2", "rep")
BLK = ("blk_0", "blk_1", "blk_2")
MESH = pl.DeviceIdType.MESH

NX, NZ, NY, NR = 4, 8, 4, 2
NP = NX * NY
NH = NP * NZ
CAP = 8
U, L, K = 8, 128, 256
ROWS = 2048
USERS = U * NH * NR
EXCHANGE_AFTER, SPREAD_AFTER = 0, 4
F32, BF16, I32 = jnp.float32, jnp.bfloat16, jnp.int32

conf_scale = 40.0
ridge = 1.0
tiny = 1e-06


def dot(a, b):
    return jnp.dot(a, b, preferred_element_type=F32)


def dot_nt(a, b):
    return lax.dot_general(a, b, (((1,), (1,)), ((), ())), preferred_element_type=F32)


def pieces(v):
    hi = v.astype(BF16)
    rest = v - hi.astype(F32)
    mid = rest.astype(BF16)
    low = (rest - mid.astype(F32)).astype(BF16)
    return hi, mid, low


def stacked(v):
    hi, mid, low = pieces(v)
    return jnp.concatenate([hi.astype(F32), mid.astype(F32), low.astype(F32)], axis=0).astype(BF16)


def folded(v, n):
    return v[:n] + v[n : 2 * n] + v[2 * n : 3 * n]


def iota(shape, dim):
    return lax.broadcasted_iota(I32, shape, dim)


class Phases:
    def __init__(self):
        self.open = None

    def __call__(self, name):
        if self.open is not None:
            self.open.__exit__(None, None, None)
        self.open = jax.named_scope(name) if name else None
        if self.open is not None:
            self.open.__enter__()


NEAR = sorted(((dx, dy) for dx in range(NX) for dy in range(NY)), key=lambda d: (min(d[0], NX - d[0]) + min(d[1], NY - d[1]), d))
EVERY = sorted(
    ((d, dz) for d in NEAR for dz in range(NZ) if d != (0, 0) or dz),
    key=lambda o: -(min(o[0][0], NX - o[0][0]) + min(o[0][1], NY - o[0][1]) + min(o[1], NZ - o[1])),
)
DIRECT = range(1, 5)
DIRECT_Z = (3, 5, 2, 6, 1, 7, 0)
GROUPS = (
    [(0, dz) for dz in (4, 3, 5, 2, 6, 1, 7, 0)],
    [(k, dz) for dz in DIRECT_Z for k in DIRECT],
    *([(k, dz) for dz in (4, 3, 5, 2, 6, 1, 7, 0) for k in (*more, *tiles) if dz == 4 or k in tiles]
      for tiles, more in ((range(5, 8), DIRECT), (range(14, 16), ()), (range(11, 14), ()), (range(8, 11), ()))),
)
FAR_Z = (4, 3, 5, 2, 6, 1, 7, 0)


def hops(d, dz):
    return min(d[0], NX - d[0]) + min(d[1], NY - d[1]) + min(dz, NZ - dz)


def direct_slot(k, dz):
    return (k - DIRECT[0]) * len(DIRECT_Z) + DIRECT_Z.index(dz)


def kernel(
    counts_hbm,
    lists_hbm,
    plays_hbm,
    users_hbm,
    items_hbm,
    out_ref,
    norms_ref,
    counts_ref,
    lists_ref,
    plays_ref,
    users_ref,
    items,
    req_send,
    req_z,
    req_near,
    req_near_t,
    req_fwd,
    req_p,
    gram_mine,
    gram_p,
    gram_zsend,
    gram_z,
    gram_red,
    gram_full,
    gram3,
    rows_send,
    rows_in,
    rows_t,
    norm_send,
    norm_pair,
    norm_mid,
    norm_all,
    local_sems,
    req_sems,
    req_near_recv,
    req_recv,
    gram_sems,
    rows_sem,
    rows_recv,
    norm_sems,
):
    phase = Phases()
    phase("enter")
    x, z, y, r = (lax.axis_index(a) for a in BLK_REP)
    p = x * NY + y

    def plane_device(d, same=1):
        return ((x + d[0]) & (NX - 1), z, (y + d[1]) & (NY - 1), r if same else 1 - r)

    def device(d, dz):
        return ((x + d[0]) & (NX - 1), (z + dz) & (NZ - 1), (y + d[1]) & (NY - 1), r)

    def z_device(dz):
        return (x, (z + dz) & (NZ - 1), y, r)

    def place_of(dev):
        return dev[0] * NY + dev[2]

    peers = [(d, same) for same in (1, 0) for d in reversed(NEAR) if not (same and d == (0, 0))]

    def send(src, dst, send_sem, recv_sem, dev):
        pltpu.make_async_remote_copy(
            src_ref=src, dst_ref=dst, send_sem=send_sem, recv_sem=recv_sem, device_id=dev, device_id_type=MESH
        ).start()

    def wait_bytes(ref, sem):
        pltpu.make_async_copy(ref, ref, sem).wait()

    copies = [
        pltpu.make_async_copy(src, dst, local_sems.at[k])
        for k, (src, dst) in enumerate(
            [(counts_hbm, counts_ref), (lists_hbm, lists_ref), (plays_hbm, plays_ref), (users_hbm, users_ref), (items_hbm, items)]
        )
    ]
    barrier = pltpu.get_barrier_semaphore()
    greeted = [((0, 0), dz, 1) for dz in range(1, NZ)] + [(d, 0, same) for d, same in peers]
    greeted += [(NEAR[k], dz, 1) for k in DIRECT for dz in DIRECT_Z[:-1]]
    for d, dz, same in sorted(greeted, key=lambda o: -hops(o[0], o[1])):
        dev = (*device(d, dz)[:3], r if same else 1 - r)
        pl.semaphore_signal(barrier, inc=1, device_id=dev, device_id_type=MESH)
    for copy in copies:
        copy.start()
    for copy in copies[:3]:
        copy.wait()

    phase("pack")
    lists = lists_ref[...]
    user = iota((U, L), 0)
    count = jnp.zeros((U, L), I32)
    for u in range(U):
        count = jnp.where(user == u, counts_ref[u], count)
    live = iota((U, L), 1) < count
    block = lists >> 11
    holder = ((block >> 2) & 7) * NP + (block >> 5) * NY + (block & 3)
    local = lists & (ROWS - 1)
    holder = jnp.where(live, holder, -1)
    before = jnp.where((iota((L, 2 * L), 0) < iota((L, 2 * L), 1)) | (iota((L, 2 * L), 1) >= L), 1.0, 0.0).astype(BF16)
    base = jnp.zeros((NH, L), F32)
    ranks = []
    for u in range(U):
        hit = jnp.where(iota((NH, L), 0) == holder[u : u + 1, :], 1.0, 0.0)
        sums = dot(hit.astype(BF16), before)
        ranks.append(jnp.sum(hit * (sums[:, :L] + base), axis=0, keepdims=True))
        base = base + sums[:, L:]
    rank = jnp.concatenate(ranks, axis=0)
    place = jnp.where(live, holder.astype(F32) * CAP + rank, -1.0)
    place_t = jnp.concatenate([place, jnp.zeros((L - U, L), F32)], axis=0).T

    phase("weights")
    confidence = 1.0 + conf_scale * jnp.log(2.0 + plays_ref[...].astype(F32))
    full_weight = jnp.where(live, confidence, 0.0)
    full3 = [v.astype(F32) for v in pieces(full_weight)]
    id_hi = (local >> 4).astype(F32)
    id_lo = (local & 15).astype(F32)
    found = jnp.zeros((4 * U, NH * CAP), F32)
    for u in range(U):
        pick = jnp.where(place_t[:, u : u + 1] == iota((L, NH * CAP), 1).astype(F32), 1.0, 0.0).astype(BF16)
        names = jnp.where(user == 0, id_hi[u : u + 1, :], jnp.where(user == 1, id_lo[u : u + 1, :], 0.0))
        left = jnp.concatenate([jnp.where(user == u, v, 0.0) for v in full3] + [names], axis=0).astype(BF16)
        found = found + dot(left, pick)
    weight = folded(found, U)
    extra = jnp.where(weight > 0.0, weight - 1.0, 0.0)
    wanted = found[3 * U : 3 * U + 1] * 16.0 + found[3 * U + 1 : 3 * U + 2]
    for k in range(NZ):
        req_send[k] = wanted[:, k * L : (k + 1) * L]
    req_z[0] = req_send[z]

    phase("barrier")
    pl.semaphore_wait(barrier, len(greeted))
    for dz in FAR_Z[:-1]:
        dev = z_device(dz)
        send(req_send.at[dev[1]], req_z.at[NZ - dz], req_sems.at[0], req_sems.at[1], dev)
    for dz in DIRECT_Z:
        for k in DIRECT:
            dev = device(NEAR[k], dz)
            at = direct_slot(k, (NZ - dz) % NZ)
            send(req_send.at[dev[1]], req_near.at[at], req_sems.at[0], req_near_recv, dev)

    phase("gram")
    copies[4].wait()
    half = pl.ds(pl.multiple_of(r * (K // NR), K // NR), K // NR)
    part = lax.dot_general(items[:, half], items[...], (((0,), (0,)), ((), ())), preferred_element_type=F32)
    gram_mine[...] = part.reshape(NP, 8, K)
    gram_p[p] = gram_mine[p]
    phase("gram_p_send")
    for d in reversed(NEAR[1:]):
        dev = plane_device(d)
        send(gram_mine.at[place_of(dev)], gram_p.at[p], gram_sems.at[0], gram_sems.at[1], dev)

    phase("req_z_wait")
    wait_bytes(req_z.at[pl.ds(0, NZ - 1)], req_sems.at[1])
    req_fwd[...] = jnp.concatenate([req_z[...].reshape(NZ, L), jnp.zeros((L - NZ, L), F32)], axis=0).T.reshape(NP, CAP, L)
    phase("req_p_send")
    for k in reversed(range(1, NP)):
        dev = plane_device(NEAR[k])
        send(req_fwd.at[place_of(dev)], req_p.at[k], req_sems.at[2], req_recv.at[k], dev)

    def exchange_gram():
        wait_bytes(gram_p.at[pl.ds(0, NP - 1)], gram_sems.at[1])
        gram_zsend[...] = jnp.sum(gram_p[...], axis=0)
        gram_z[z] = gram_zsend[...]
        for dz in FAR_Z[:-1]:
            send(gram_zsend, gram_z.at[z], gram_sems.at[2], gram_sems.at[3], z_device(dz))

    def spread_gram():
        wait_bytes(gram_z.at[pl.ds(0, NZ - 1)], gram_sems.at[3])
        gram_red[...] = jnp.sum(gram_z[...], axis=0)
        gram_full[r * NP + p] = gram_red[...]
        for d, same in peers:
            send(gram_red, gram_full.at[r * NP + p], gram_sems.at[4], gram_sems.at[5], plane_device(d, same))

    def serve(first, goals):
        direct = goals is GROUPS[1]
        if direct:
            wait_bytes(req_near, req_near_recv)
            known = len(DIRECT) * len(DIRECT_Z)
            near = jnp.concatenate([req_near[...].reshape(known, L), jnp.zeros((L - known, L), F32)], axis=0).T
            req_near_t[...] = near.reshape(NP, CAP, L)
            near = req_near_t[p]
            columns = [near[:, direct_slot(k, dz) : direct_slot(k, dz) + 1] for k, dz in goals]
        else:
            tiles = {}
            for k in sorted({k for k, _ in goals}):
                if k:
                    wait_bytes(req_p.at[k], req_recv.at[k])
                tiles[k] = req_p[k] if k else req_fwd[p]
            columns = [tiles[k][:, dz : dz + 1] for k, dz in goals]
        column = jnp.concatenate(columns, axis=0)
        count = len(goals) * CAP
        total = jnp.zeros((count, K), F32)
        width = 512
        for part in range(ROWS // width):
            pick = jnp.where(column == (iota((count, width), 1) + part * width).astype(F32), 1.0, 0.0).astype(BF16)
            total = total + dot(pick, items[part * width : (part + 1) * width, :])
        rows_send[first : first + len(goals)] = total.reshape(len(goals), CAP, K).astype(BF16)
        for i, (k, dz) in enumerate(goals):
            d = NEAR[k]
            dev = ((x - d[0]) & (NX - 1), (z + dz) & (NZ - 1), (y - d[1]) & (NY - 1), r)
            src = rows_send.at[first + i]
            dst = rows_in.at[pl.ds(pl.multiple_of((z * NP + p) * CAP, CAP), CAP), :]
            if k == 0 and dz == 0:
                pltpu.make_async_copy(src, dst, rows_recv).start()
            else:
                send(src, dst, rows_sem, rows_recv, dev)
        return first + len(goals)

    served = 0
    for n, goals in enumerate(GROUPS):
        phase("serve%d" % n)
        served = serve(served, goals)
        if n == EXCHANGE_AFTER:
            phase("gram_z")
            exchange_gram()
        if n == SPREAD_AFTER:
            phase("gram_ag")
            spread_gram()

    phase("gram_ag_wait")
    wait_bytes(gram_full.at[pl.ds(0, NP * NR - 1)], gram_sems.at[5])
    phase("gram_pieces")
    for k, piece in enumerate(pieces(gram_full[...].reshape(K, K))):
        gram3[:, k * K : (k + 1) * K] = piece

    def gram_part(v3):
        g = folded(dot(v3, gram3[...]), U)
        return g[:, :K] + g[:, K : 2 * K] + g[:, 2 * K :]

    copies[3].wait()
    start = users_ref[...]
    start3 = stacked(start)
    start_image = gram_part(start3) + ridge * start
    weight3 = stacked(weight)

    phase("rows_wait")
    wait_bytes(rows_in, rows_recv)

    phase("cg")
    def image_of(v):
        v3 = stacked(v)
        along = folded(dot(v3, rows_t[...]), U)
        back = folded(dot(stacked(extra * along), rows_in[...]), U)
        return gram_part(v3) + back + ridge * v

    def inner(a, b):
        return jnp.sum(a * b, axis=1, keepdims=True)

    rows_t[...] = rows_in[...].T
    along = folded(dot(start3, rows_t[...]), U)
    both = dot(jnp.concatenate([weight3.astype(F32), stacked(extra * along).astype(F32)], axis=0).astype(BF16), rows_in[...])
    solution = start
    residual = folded(both[: 3 * U], U) - (start_image + folded(both[3 * U :], U))
    direction = residual
    squares = inner(residual, residual)
    lane = iota((U, L), 1)
    collected = jnp.where(lane == 0, squares, 0.0)
    for t in range(ITERS):
        image = image_of(direction)
        alpha = squares / (inner(direction, image) + tiny)
        solution = solution + alpha * direction
        residual = residual - alpha * image
        fresh = inner(residual, residual)
        direction = residual + (fresh / (squares + tiny)) * direction
        squares = fresh
        collected = collected + jnp.where(lane == t + 1, squares, 0.0)

    norm_send[...] = jnp.sum(collected, axis=0, keepdims=True)
    phase("norm_pair")
    norm_pair[r] = norm_send[...]
    send(norm_send, norm_pair.at[r], norm_sems.at[0], norm_sems.at[1], plane_device((0, 0), 0))
    out_ref[...] = solution
    wait_bytes(req_z.at[pl.ds(0, NZ - 1)], req_sems.at[0])
    wait_bytes(req_near, req_sems.at[0])
    wait_bytes(req_p.at[pl.ds(0, NP - 1)], req_sems.at[2])
    wait_bytes(gram_mine.at[pl.ds(0, NP - 1)], gram_sems.at[0])
    wait_bytes(gram_z.at[pl.ds(0, NZ - 1)], gram_sems.at[2])
    wait_bytes(gram_full.at[pl.ds(0, NP * NR - 1)], gram_sems.at[4])
    wait_bytes(rows_send.at[pl.ds(0, NH - 1)], rows_sem)
    wait_bytes(norm_pair.at[pl.ds(0, 1)], norm_sems.at[1])
    norm_mid[...] = norm_pair[0] + norm_pair[1]
    phase("norm_all")
    norm_all[z * NP + p] = norm_mid[...]
    for d, dz in EVERY:
        dev = ((x + d[0]) & (NX - 1), (z + dz) & (NZ - 1), (y + d[1]) & (NY - 1), 1 - r)
        send(norm_mid, norm_all.at[z * NP + p], norm_sems.at[2], norm_sems.at[3], dev)
    wait_bytes(norm_pair.at[pl.ds(0, 1)], norm_sems.at[0])
    wait_bytes(norm_all.at[pl.ds(0, NH - 1)], norm_sems.at[3])
    phase("norm_end")
    total = jnp.sum(norm_all[...], axis=0)
    norms_ref[...] = jnp.sqrt(total / (USERS * K))[:, : ITERS + 1]
    wait_bytes(norm_all.at[pl.ds(0, NH - 1)], norm_sems.at[2])
    phase(None)


def put_out(factors, norms, factors_out, norms_out, sems):
    copies = [pltpu.make_async_copy(factors, factors_out, sems.at[0]), pltpu.make_async_copy(norms, norms_out, sems.at[1])]
    for copy in copies:
        copy.start()
    for copy in copies:
        copy.wait()


def body(item_factors, user_factors, item_lists, counts, plays):
    vmem = pl.BlockSpec(memory_space=pltpu.VMEM)
    dma = pltpu.SemaphoreType.DMA
    new_factors, norms = pl.pallas_call(
        kernel,
        out_shape=(pltpu.VMEM((U, K), F32), pltpu.VMEM((1, ITERS + 1), F32)),
        in_specs=[pl.BlockSpec(memory_space=pltpu.HBM)] * 5,
        out_specs=(vmem, vmem),
        scratch_shapes=[
            pltpu.SMEM((U,), I32),
            pltpu.VMEM((U, L), I32),
            pltpu.VMEM((U, L), I32),
            pltpu.VMEM((U, K), F32),
            pltpu.VMEM((ROWS, K), BF16),
            pltpu.VMEM((NZ, 1, L), F32),
            pltpu.VMEM((NZ, 1, L), F32),
            pltpu.VMEM((len(DIRECT) * len(DIRECT_Z), 1, L), F32),
            pltpu.VMEM((NP, CAP, L), F32),
            pltpu.VMEM((NP, CAP, L), F32),
            pltpu.VMEM((NP, CAP, L), F32),
            pltpu.VMEM((NP, 8, K), F32),
            pltpu.VMEM((NP, 8, K), F32),
            pltpu.VMEM((8, K), F32),
            pltpu.VMEM((NZ, 8, K), F32),
            pltpu.VMEM((8, K), F32),
            pltpu.VMEM((NR * NP, 8, K), F32),
            pltpu.VMEM((K, 3 * K), BF16),
            pltpu.VMEM((NP * NZ, CAP, K), BF16),
            pltpu.VMEM((NH * CAP, K), BF16),
            pltpu.VMEM((K, NH * CAP), BF16),
            pltpu.VMEM((1, L), F32),
            pltpu.VMEM((NR, 1, L), F32),
            pltpu.VMEM((1, L), F32),
            pltpu.VMEM((NH, 1, L), F32),
            dma((5,)),
            dma((3,)),
            dma,
            dma((NP,)),
            dma((6,)),
            dma,
            dma,
            dma((4,)),
        ],
        compiler_params=pltpu.CompilerParams(collective_id=0, has_side_effects=True),
    )(counts, item_lists, plays, user_factors, item_factors)
    new_factors, norms = pl.pallas_call(
        put_out,
        out_shape=(jax.ShapeDtypeStruct((U, K), F32), jax.ShapeDtypeStruct((1, ITERS + 1), F32)),
        in_specs=[vmem, vmem],
        out_specs=(pl.BlockSpec(memory_space=pltpu.HBM), pl.BlockSpec(memory_space=pltpu.HBM)),
        scratch_shapes=[dma((2,))],
        compiler_params=pltpu.CompilerParams(vmem_limit_bytes=1024 * 1024),
    )(new_factors, norms)
    return new_factors, norms.reshape(ITERS + 1)


def solution(mesh):
    split = Mesh(mesh.devices.reshape(NX, NZ, NY, NR), BLK_REP)
    in_specs = (P(BLK, None), P(BLK_REP, None), P(BLK_REP, None), P(BLK_REP), P(BLK_REP, None))
    out_specs = (P(BLK_REP, None), P())
    return jax.shard_map(body, mesh=split, in_specs=in_specs, out_specs=out_specs, check_vma=False)
```

```python
import jax
import jax.numpy as jnp
from jax import lax
from jax.experimental import pallas as pl
from jax.experimental.pallas import tpu as pltpu
from jax.sharding import Mesh
from jax.sharding import PartitionSpec as P

ITERS = 3
BLK_REP = ("blk_0", "blk_1", "blk_2", "rep")
BLK = ("blk_0", "blk_1", "blk_2")
MESH = pl.DeviceIdType.MESH

NX, NZ, NY, NR = 4, 8, 4, 2
NP = NX * NY
NH = NP * NZ
CAP = 8
U, L, K = 8, 128, 256
ROWS = 2048
USERS = U * NH * NR
EXCHANGE_AFTER, SPREAD_AFTER = 0, 5
F32, BF16, I32 = jnp.float32, jnp.bfloat16, jnp.int32

conf_scale = 40.0
ridge = 1.0
tiny = 1e-06


def dot(a, b):
    return jnp.dot(a, b, preferred_element_type=F32)


def dot_nt(a, b):
    return lax.dot_general(a, b, (((1,), (1,)), ((), ())), preferred_element_type=F32)


def pieces(v):
    hi = v.astype(BF16)
    rest = v - hi.astype(F32)
    mid = rest.astype(BF16)
    low = (rest - mid.astype(F32)).astype(BF16)
    return hi, mid, low


def stacked(v):
    hi, mid, low = pieces(v)
    return jnp.concatenate([hi.astype(F32), mid.astype(F32), low.astype(F32)], axis=0).astype(BF16)


def folded(v, n):
    return v[:n] + v[n : 2 * n] + v[2 * n : 3 * n]


def iota(shape, dim):
    return lax.broadcasted_iota(I32, shape, dim)


class Phases:
    def __init__(self):
        self.open = None

    def __call__(self, name):
        if self.open is not None:
            self.open.__exit__(None, None, None)
        self.open = jax.named_scope(name) if name else None
        if self.open is not None:
            self.open.__enter__()


NEAR = sorted(((dx, dy) for dx in range(NX) for dy in range(NY)), key=lambda d: (min(d[0], NX - d[0]) + min(d[1], NY - d[1]), d))
EVERY = sorted(
    ((d, dz) for d in NEAR for dz in range(NZ) if d != (0, 0) or dz),
    key=lambda o: -(min(o[0][0], NX - o[0][0]) + min(o[0][1], NY - o[0][1]) + min(o[1], NZ - o[1])),
)
DIRECT = range(1, 5)
DIRECT_Z = (3, 5, 2, 6, 1, 7, 0)
GROUPS = (
    [(0, dz) for dz in (4, 3, 5, 2, 6, 1, 7, 0)],
    [(k, dz) for dz in DIRECT_Z for k in DIRECT],
    *([(k, dz) for dz in (4, 3, 5, 2, 6, 1, 7, 0) for k in (*more, *tiles) if dz == 4 or k in tiles]
      for tiles, more in ((range(5, 8), DIRECT), (range(14, 16), ()), (range(11, 14), ()), (range(8, 11), ()))),
)
FAR_Z = (4, 3, 5, 2, 6, 1, 7, 0)


def hops(d, dz):
    return min(d[0], NX - d[0]) + min(d[1], NY - d[1]) + min(dz, NZ - dz)


def direct_slot(k, dz):
    return (k - DIRECT[0]) * len(DIRECT_Z) + DIRECT_Z.index(dz)


def kernel(
    counts_hbm,
    lists_hbm,
    plays_hbm,
    users_hbm,
    items_hbm,
    out_ref,
    norms_ref,
    counts_ref,
    lists_ref,
    plays_ref,
    users_ref,
    items,
    req_send,
    req_z,
    req_near,
    req_near_t,
    req_fwd,
    req_p,
    gram_mine,
    gram_p,
    gram_zsend,
    gram_z,
    gram_red,
    gram_full,
    gram3,
    rows_send,
    rows_in,
    norm_send,
    norm_pair,
    norm_mid,
    norm_all,
    local_sems,
    req_sems,
    req_near_recv,
    req_recv,
    gram_sems,
    rows_sem,
    rows_recv,
    norm_sems,
):
    phase = Phases()
    phase("enter")
    x, z, y, r = (lax.axis_index(a) for a in BLK_REP)
    p = x * NY + y

    def plane_device(d, same=1):
        return ((x + d[0]) & (NX - 1), z, (y + d[1]) & (NY - 1), r if same else 1 - r)

    def device(d, dz):
        return ((x + d[0]) & (NX - 1), (z + dz) & (NZ - 1), (y + d[1]) & (NY - 1), r)

    def z_device(dz):
        return (x, (z + dz) & (NZ - 1), y, r)

    def place_of(dev):
        return dev[0] * NY + dev[2]

    peers = [(d, same) for same in (1, 0) for d in reversed(NEAR) if not (same and d == (0, 0))]

    def send(src, dst, send_sem, recv_sem, dev):
        pltpu.make_async_remote_copy(
            src_ref=src, dst_ref=dst, send_sem=send_sem, recv_sem=recv_sem, device_id=dev, device_id_type=MESH
        ).start()

    def wait_bytes(ref, sem):
        pltpu.make_async_copy(ref, ref, sem).wait()

    copies = [
        pltpu.make_async_copy(src, dst, local_sems.at[k])
        for k, (src, dst) in enumerate(
            [(counts_hbm, counts_ref), (lists_hbm, lists_ref), (plays_hbm, plays_ref), (users_hbm, users_ref), (items_hbm, items)]
        )
    ]
    for copy in copies:
        copy.start()
    barrier = pltpu.get_barrier_semaphore()
    greeted = [((0, 0), dz, 1) for dz in range(1, NZ)] + [(d, 0, same) for d, same in peers]
    greeted += [(NEAR[k], dz, 1) for k in DIRECT for dz in DIRECT_Z[:-1]]
    for d, dz, same in sorted(greeted, key=lambda o: -hops(o[0], o[1])):
        dev = (*device(d, dz)[:3], r if same else 1 - r)
        pl.semaphore_signal(barrier, inc=1, device_id=dev, device_id_type=MESH)
    for copy in copies[:3]:
        copy.wait()

    phase("pack")
    lists = lists_ref[...]
    user = iota((U, L), 0)
    count = jnp.zeros((U, L), I32)
    for u in range(U):
        count = jnp.where(user == u, counts_ref[u], count)
    live = iota((U, L), 1) < count
    block = lists >> 11
    holder = ((block >> 2) & 7) * NP + (block >> 5) * NY + (block & 3)
    local = lists & (ROWS - 1)
    holder = jnp.where(live, holder, -1)
    before = jnp.where((iota((L, 2 * L), 0) < iota((L, 2 * L), 1)) | (iota((L, 2 * L), 1) >= L), 1.0, 0.0).astype(BF16)
    base = jnp.zeros((NH, L), F32)
    ranks = []
    for u in range(U):
        hit = jnp.where(iota((NH, L), 0) == holder[u : u + 1, :], 1.0, 0.0)
        sums = dot(hit.astype(BF16), before)
        ranks.append(jnp.sum(hit * (sums[:, :L] + base), axis=0, keepdims=True))
        base = base + sums[:, L:]
    rank = jnp.concatenate(ranks, axis=0)
    place = jnp.where(live, holder.astype(F32) * CAP + rank, -1.0)
    place_t = jnp.concatenate([place, jnp.zeros((L - U, L), F32)], axis=0).T

    phase("weights")
    confidence = 1.0 + conf_scale * jnp.log(2.0 + plays_ref[...].astype(F32))
    full_weight = jnp.where(live, confidence, 0.0)
    full3 = [v.astype(F32) for v in pieces(full_weight)]
    id_hi = (local >> 4).astype(F32)
    id_lo = (local & 15).astype(F32)
    found = jnp.zeros((4 * U, NH * CAP), F32)
    for u in range(U):
        pick = jnp.where(place_t[:, u : u + 1] == iota((L, NH * CAP), 1).astype(F32), 1.0, 0.0).astype(BF16)
        names = jnp.where(user == 0, id_hi[u : u + 1, :], jnp.where(user == 1, id_lo[u : u + 1, :], 0.0))
        left = jnp.concatenate([jnp.where(user == u, v, 0.0) for v in full3] + [names], axis=0).astype(BF16)
        found = found + dot(left, pick)
    weight = folded(found, U)
    extra = jnp.where(weight > 0.0, weight - 1.0, 0.0)
    wanted = found[3 * U : 3 * U + 1] * 16.0 + found[3 * U + 1 : 3 * U + 2]
    for k in range(NZ):
        req_send[k] = wanted[:, k * L : (k + 1) * L]
    req_z[0] = req_send[z]

    phase("barrier")
    pl.semaphore_wait(barrier, len(greeted))
    for dz in FAR_Z[:-1]:
        dev = z_device(dz)
        send(req_send.at[dev[1]], req_z.at[NZ - dz], req_sems.at[0], req_sems.at[1], dev)
    for dz in DIRECT_Z:
        for k in DIRECT:
            dev = device(NEAR[k], dz)
            at = direct_slot(k, (NZ - dz) % NZ)
            send(req_send.at[dev[1]], req_near.at[at], req_sems.at[0], req_near_recv, dev)

    phase("gram")
    copies[4].wait()
    half = pl.ds(pl.multiple_of(r * (K // NR), K // NR), K // NR)
    part = lax.dot_general(items[:, half], items[...], (((0,), (0,)), ((), ())), preferred_element_type=F32)
    gram_mine[...] = part.reshape(NP, 8, K)
    gram_p[p] = gram_mine[p]
    phase("gram_p_send")
    for d in reversed(NEAR[1:]):
        dev = plane_device(d)
        send(gram_mine.at[place_of(dev)], gram_p.at[p], gram_sems.at[0], gram_sems.at[1], dev)

    phase("req_z_wait")
    wait_bytes(req_z.at[pl.ds(0, NZ - 1)], req_sems.at[1])
    req_fwd[...] = jnp.concatenate([req_z[...].reshape(NZ, L), jnp.zeros((L - NZ, L), F32)], axis=0).T.reshape(NP, CAP, L)
    phase("req_p_send")
    for k in reversed(range(1, NP)):
        dev = plane_device(NEAR[k])
        send(req_fwd.at[place_of(dev)], req_p.at[k], req_sems.at[2], req_recv.at[k], dev)

    def exchange_gram():
        wait_bytes(gram_p.at[pl.ds(0, NP - 1)], gram_sems.at[1])
        gram_zsend[...] = jnp.sum(gram_p[...], axis=0)
        gram_z[z] = gram_zsend[...]
        for dz in FAR_Z[:-1]:
            send(gram_zsend, gram_z.at[z], gram_sems.at[2], gram_sems.at[3], z_device(dz))

    def spread_gram():
        wait_bytes(gram_z.at[pl.ds(0, NZ - 1)], gram_sems.at[3])
        gram_red[...] = jnp.sum(gram_z[...], axis=0)
        gram_full[r * NP + p] = gram_red[...]
        for d, same in peers:
            send(gram_red, gram_full.at[r * NP + p], gram_sems.at[4], gram_sems.at[5], plane_device(d, same))

    def serve(first, goals):
        direct = goals is GROUPS[1]
        if direct:
            wait_bytes(req_near, req_near_recv)
            known = len(DIRECT) * len(DIRECT_Z)
            near = jnp.concatenate([req_near[...].reshape(known, L), jnp.zeros((L - known, L), F32)], axis=0).T
            req_near_t[...] = near.reshape(NP, CAP, L)
            near = req_near_t[p]
            columns = [near[:, direct_slot(k, dz) : direct_slot(k, dz) + 1] for k, dz in goals]
        else:
            tiles = {}
            for k in sorted({k for k, _ in goals}):
                if k:
                    wait_bytes(req_p.at[k], req_recv.at[k])
                tiles[k] = req_p[k] if k else req_fwd[p]
            columns = [tiles[k][:, dz : dz + 1] for k, dz in goals]
        column = jnp.concatenate(columns, axis=0)
        count = len(goals) * CAP
        total = jnp.zeros((count, K), F32)
        width = 512
        for part in range(ROWS // width):
            pick = jnp.where(column == (iota((count, width), 1) + part * width).astype(F32), 1.0, 0.0).astype(BF16)
            total = total + dot(pick, items[part * width : (part + 1) * width, :])
        rows_send[first : first + len(goals)] = total.reshape(len(goals), CAP, K).astype(BF16)
        for i, (k, dz) in enumerate(goals):
            d = NEAR[k]
            dev = ((x - d[0]) & (NX - 1), (z + dz) & (NZ - 1), (y - d[1]) & (NY - 1), r)
            src = rows_send.at[first + i]
            dst = rows_in.at[pl.ds(pl.multiple_of((z * NP + p) * CAP, CAP), CAP), :]
            if k == 0 and dz == 0:
                pltpu.make_async_copy(src, dst, rows_recv).start()
            else:
                send(src, dst, rows_sem, rows_recv, dev)
        return first + len(goals)

    served = 0
    for n, goals in enumerate(GROUPS):
        phase("serve%d" % n)
        served = serve(served, goals)
        if n == EXCHANGE_AFTER:
            phase("gram_z")
            exchange_gram()
        if n == SPREAD_AFTER:
            phase("gram_ag")
            spread_gram()

    phase("gram_ag_wait")
    wait_bytes(gram_full.at[pl.ds(0, NP * NR - 1)], gram_sems.at[5])
    phase("gram_pieces")
    for k, piece in enumerate(pieces(gram_full[...].reshape(K, K))):
        gram3[:, k * K : (k + 1) * K] = piece

    def gram_part(v3):
        g = folded(dot(v3, gram3[...]), U)
        return g[:, :K] + g[:, K : 2 * K] + g[:, 2 * K :]

    copies[3].wait()
    start = users_ref[...]
    start3 = stacked(start)
    start_image = gram_part(start3) + ridge * start
    weight3 = stacked(weight)

    phase("rows_wait")
    wait_bytes(rows_in, rows_recv)

    phase("cg")
    def image_of(v):
        v3 = stacked(v)
        along = folded(dot_nt(v3, rows_in[...]), U)
        back = folded(dot(stacked(extra * along), rows_in[...]), U)
        return gram_part(v3) + back + ridge * v

    def inner(a, b):
        return jnp.sum(a * b, axis=1, keepdims=True)

    along = folded(dot_nt(start3, rows_in[...]), U)
    both = dot(jnp.concatenate([weight3.astype(F32), stacked(extra * along).astype(F32)], axis=0).astype(BF16), rows_in[...])
    solution = start
    residual = folded(both[: 3 * U], U) - (start_image + folded(both[3 * U :], U))
    direction = residual
    squares = inner(residual, residual)
    lane = iota((U, L), 1)
    collected = jnp.where(lane == 0, squares, 0.0)
    for t in range(ITERS):
        image = image_of(direction)
        alpha = squares / (inner(direction, image) + tiny)
        solution = solution + alpha * direction
        residual = residual - alpha * image
        fresh = inner(residual, residual)
        direction = residual + (fresh / (squares + tiny)) * direction
        squares = fresh
        collected = collected + jnp.where(lane == t + 1, squares, 0.0)

    norm_send[...] = jnp.sum(collected, axis=0, keepdims=True)
    phase("norm_pair")
    norm_pair[r] = norm_send[...]
    send(norm_send, norm_pair.at[r], norm_sems.at[0], norm_sems.at[1], plane_device((0, 0), 0))
    out_ref[...] = solution
    wait_bytes(req_z.at[pl.ds(0, NZ - 1)], req_sems.at[0])
    wait_bytes(req_near, req_sems.at[0])
    wait_bytes(req_p.at[pl.ds(0, NP - 1)], req_sems.at[2])
    wait_bytes(gram_mine.at[pl.ds(0, NP - 1)], gram_sems.at[0])
    wait_bytes(gram_z.at[pl.ds(0, NZ - 1)], gram_sems.at[2])
    wait_bytes(gram_full.at[pl.ds(0, NP * NR - 1)], gram_sems.at[4])
    wait_bytes(rows_send.at[pl.ds(0, NH - 1)], rows_sem)
    wait_bytes(norm_pair.at[pl.ds(0, 1)], norm_sems.at[1])
    norm_mid[...] = norm_pair[0] + norm_pair[1]
    phase("norm_all")
    norm_all[z * NP + p] = norm_mid[...]
    for d, dz in EVERY:
        dev = ((x + d[0]) & (NX - 1), (z + dz) & (NZ - 1), (y + d[1]) & (NY - 1), 1 - r)
        send(norm_mid, norm_all.at[z * NP + p], norm_sems.at[2], norm_sems.at[3], dev)
    wait_bytes(norm_pair.at[pl.ds(0, 1)], norm_sems.at[0])
    wait_bytes(norm_all.at[pl.ds(0, NH - 1)], norm_sems.at[3])
    phase("norm_end")
    total = jnp.sum(norm_all[...], axis=0)
    norms_ref[...] = jnp.sqrt(total / (USERS * K))[:, : ITERS + 1]
    wait_bytes(norm_all.at[pl.ds(0, NH - 1)], norm_sems.at[2])
    phase(None)


def put_out(factors, norms, factors_out, norms_out, sems):
    copies = [pltpu.make_async_copy(factors, factors_out, sems.at[0]), pltpu.make_async_copy(norms, norms_out, sems.at[1])]
    for copy in copies:
        copy.start()
    for copy in copies:
        copy.wait()


def body(item_factors, user_factors, item_lists, counts, plays):
    vmem = pl.BlockSpec(memory_space=pltpu.VMEM)
    dma = pltpu.SemaphoreType.DMA
    new_factors, norms = pl.pallas_call(
        kernel,
        out_shape=(pltpu.VMEM((U, K), F32), pltpu.VMEM((1, ITERS + 1), F32)),
        in_specs=[pl.BlockSpec(memory_space=pltpu.HBM)] * 5,
        out_specs=(vmem, vmem),
        scratch_shapes=[
            pltpu.SMEM((U,), I32),
            pltpu.VMEM((U, L), I32),
            pltpu.VMEM((U, L), I32),
            pltpu.VMEM((U, K), F32),
            pltpu.VMEM((ROWS, K), BF16),
            pltpu.VMEM((NZ, 1, L), F32),
            pltpu.VMEM((NZ, 1, L), F32),
            pltpu.VMEM((len(DIRECT) * len(DIRECT_Z), 1, L), F32),
            pltpu.VMEM((NP, CAP, L), F32),
            pltpu.VMEM((NP, CAP, L), F32),
            pltpu.VMEM((NP, CAP, L), F32),
            pltpu.VMEM((NP, 8, K), F32),
            pltpu.VMEM((NP, 8, K), F32),
            pltpu.VMEM((8, K), F32),
            pltpu.VMEM((NZ, 8, K), F32),
            pltpu.VMEM((8, K), F32),
            pltpu.VMEM((NR * NP, 8, K), F32),
            pltpu.VMEM((K, 3 * K), BF16),
            pltpu.VMEM((NP * NZ, CAP, K), BF16),
            pltpu.VMEM((NH * CAP, K), BF16),
            pltpu.VMEM((1, L), F32),
            pltpu.VMEM((NR, 1, L), F32),
            pltpu.VMEM((1, L), F32),
            pltpu.VMEM((NH, 1, L), F32),
            dma((5,)),
            dma((3,)),
            dma,
            dma((NP,)),
            dma((6,)),
            dma,
            dma,
            dma((4,)),
        ],
        compiler_params=pltpu.CompilerParams(collective_id=0, has_side_effects=True),
    )(counts, item_lists, plays, user_factors, item_factors)
    new_factors, norms = pl.pallas_call(
        put_out,
        out_shape=(jax.ShapeDtypeStruct((U, K), F32), jax.ShapeDtypeStruct((1, ITERS + 1), F32)),
        in_specs=[vmem, vmem],
        out_specs=(pl.BlockSpec(memory_space=pltpu.HBM), pl.BlockSpec(memory_space=pltpu.HBM)),
        scratch_shapes=[dma((2,))],
        compiler_params=pltpu.CompilerParams(vmem_limit_bytes=1024 * 1024),
    )(new_factors, norms)
    return new_factors, norms.reshape(ITERS + 1)


def solution(mesh):
    split = Mesh(mesh.devices.reshape(NX, NZ, NY, NR), BLK_REP)
    in_specs = (P(BLK, None), P(BLK_REP, None), P(BLK_REP, None), P(BLK_REP), P(BLK_REP, None))
    out_specs = (P(BLK_REP, None), P())
    return jax.shard_map(body, mesh=split, in_specs=in_specs, out_specs=out_specs, check_vma=False)
```
